256 devices in a mesh: ctx: 64 (over x, z, core), head: 4 (over y).
Axes of the slice: x: 4, y: 4, z: 8, core: 2. Of those that a mesh axis runs over, the one named last changes fastest.
Arguments:
- queries: bfloat16 [16384, 2048], P(('ctx', 'head')), may hold values from -6 to 6
- key_vectors_state: bfloat16 [16384, 512], P(('ctx', 'head')), may hold values from -6 to 6
- value_vectors_state: bfloat16 [16384, 512], P(('ctx', 'head')), may hold values from -6 to 6
- doc_bounds: int32 [17], replicated, may hold values from 0 to 16384, as said below
Outputs:
- attended: bfloat16 [16384, 2048], P(('ctx', 'head'))
The draws below stay inside these ranges and needn't reach their ends.
Inputs may be any that keep to these rules, and one draw needn't show every extreme that they name: doc_bounds[0] is 0 and doc_bounds[16] is 16384; the entries strictly increase, and doc_bounds[1] to doc_bounds[15] all lie below 8192, so the last document holds at least half of the tokens.
All inputs are finite; a program needn't handle non-finite values.
Results may differ from the reference program's by a relative error of at most 0.004.
Values may be sent and summed in bfloat16 or wider, within the bound.
No kernel may reach another device: no remote copies, remote signals or barrier semaphores. Data moves between devices by JAX's collectives and lax.ppermute only.
A program may use at most 64 MiB of HBM per device.

```python
import math
import jax
import jax.numpy as jnp
from jax import lax

QUERY_HEADS = 32
KEY_VALUE_HEADS = 8
HEAD_SIZE = 64
DOCS = 16
PACKED_TOKENS = 16384


def draw_queries(key, part):
    base_value = jax.random.fold_in(key, 21)
    drawn_sample = jnp.clip(jax.random.normal(base_value, (PACKED_TOKENS, QUERY_HEADS * HEAD_SIZE), jnp.float32), -6.0, 6.0)
    return drawn_sample.astype(jnp.bfloat16)


def draw_key_vectors_state(key, part):
    base_value = jax.random.fold_in(key, 22)
    drawn_sample = jnp.clip(jax.random.normal(base_value, (PACKED_TOKENS, KEY_VALUE_HEADS * HEAD_SIZE), jnp.float32), -6.0, 6.0)
    return drawn_sample.astype(jnp.bfloat16)


def draw_doc_bounds(key, part):
    cuts = jax.random.permutation(jax.random.fold_in(key, 31), PACKED_TOKENS // 2 - 1)[:DOCS - 1] + 1
    cuts = jnp.sort(cuts.astype(jnp.int32))
    return jnp.concatenate([jnp.zeros((1,), jnp.int32), cuts, jnp.full((1,), PACKED_TOKENS, jnp.int32)])


def block_levels(own_key, dims, split, low, high):
    def one(position, shards_of):
        draws = jax.random.uniform(jax.random.fold_in(jax.random.fold_in(own_key, 6), position), (shards_of,), jnp.float32, low / len(split), high / len(split))
        return jnp.repeat(jnp.exp(draws), dims[position] // shards_of).reshape((-1,) + (1,) * (len(dims) - position - 1))

    factor_of = one(*split[0])
    for cut in split[1:]:
        factor_of = factor_of * one(*cut)
    return factor_of


def centred(rng, dims, deviation, reach, shards=(), held_as=jnp.bfloat16):
    drawn = deviation * jax.random.normal(rng, dims, jnp.float32)
    if shards:
        drawn = drawn * block_levels(rng, dims, shards, -0.22, 0.18)
    return jnp.clip(drawn, -reach, reach).astype(held_as)


def setup_inputs(seed: int = 0) -> dict:
    streams_of = jax.random.split(jax.random.key(seed), 5)
    return {
        "queries": draw_queries(jax.random.fold_in(streams_of[4], 71), 0),
        "key_vectors_state": draw_key_vectors_state(jax.random.fold_in(streams_of[4], 71), 0),
        "value_vectors_state": centred(streams_of[2], (PACKED_TOKENS, KEY_VALUE_HEADS * HEAD_SIZE), 1.0, 6.0, ((0, 256),)),
        "doc_bounds": draw_doc_bounds(jax.random.fold_in(streams_of[4], 71), 0),
    }


masked_score = -1e+30

def document_of(positions, doc_bounds):
    interior = doc_bounds[1:-1]
    return lax.optimization_barrier(jnp.sum((interior[None, :] <= positions[:, None]).astype(jnp.int32), axis=1))

def reference(queries, key_vectors_state, value_vectors_state, doc_bounds):
    sequence_length = queries.shape[0]
    queries_per_group = QUERY_HEADS // KEY_VALUE_HEADS
    score_scale = 1.0 / math.sqrt(HEAD_SIZE)
    heads_of_queries = queries.reshape(sequence_length, KEY_VALUE_HEADS, queries_per_group, HEAD_SIZE)
    heads_of_keys = key_vectors_state.reshape(sequence_length, KEY_VALUE_HEADS, HEAD_SIZE)
    heads_of_values = value_vectors_state.reshape(sequence_length, KEY_VALUE_HEADS, HEAD_SIZE)
    positions = jnp.arange(sequence_length, dtype=jnp.int32)
    doc_ids = document_of(positions, doc_bounds)
    row_block = min(512, sequence_length)
    num_blocks = sequence_length // row_block

    def one_block(block_index):
        anchor = (block_index * row_block).astype(jnp.int32)
        query_block = lax.dynamic_slice_in_dim(heads_of_queries, anchor, row_block, 0)
        query_pos = anchor + jnp.arange(row_block, dtype=jnp.int32)
        query_doc = lax.dynamic_slice_in_dim(doc_ids, anchor, row_block, 0)
        allowed = (query_doc[:, None] == doc_ids[None, :]) & (positions[None, :] <= query_pos[:, None])
        visible = allowed[:, None, :]

        def single_head(head_index):
            query_group = lax.dynamic_index_in_dim(query_block, head_index, 1, keepdims=False)
            key_group = lax.dynamic_index_in_dim(heads_of_keys, head_index, 1, keepdims=False)
            value_group = lax.dynamic_index_in_dim(heads_of_values, head_index, 1, keepdims=False)
            scores = jnp.einsum('qjd,kd->qjk', query_group.astype(jnp.float32), key_group.astype(jnp.float32)) * score_scale
            masked = jnp.where(visible, scores, masked_score)
            top_score = lax.optimization_barrier(jnp.max(masked, axis=-1))
            weights = jnp.exp(masked - top_score[..., None]) * visible.astype(jnp.float32)
            weight_sum = lax.optimization_barrier(jnp.sum(weights, axis=-1))
            rounded = lax.optimization_barrier(weights.astype(jnp.bfloat16))
            mixed = jnp.einsum('qjk,kd->qjd', rounded.astype(jnp.float32), value_group.astype(jnp.float32))
            return (mixed / weight_sum[..., None]).astype(jnp.bfloat16)
        output_heads = lax.map(single_head, jnp.arange(KEY_VALUE_HEADS, dtype=jnp.int32))
        return jnp.transpose(output_heads, (1, 0, 2, 3))
    blocks_out = lax.map(one_block, jnp.arange(num_blocks, dtype=jnp.int32))
    return blocks_out.reshape(sequence_length, QUERY_HEADS * HEAD_SIZE)
```

```python
import functools
import math

import jax
import jax.numpy as jnp
from jax import lax
from jax.experimental import pallas as pl
from jax.experimental.pallas import tpu as pltpu
from jax.sharding import Mesh, PartitionSpec as P

QUERY_HEADS = 32
KEY_VALUE_HEADS = 8
HEAD_SIZE = 64
GROUP = QUERY_HEADS // KEY_VALUE_HEADS

X, Z, CORES, Y = 4, 8, 2, 4
BLOCK = 64
TILE = 256
STEP_TILES = 4
PAIR = 2
ROWS = PAIR * GROUP * BLOCK

EXP2_SCALE = math.log2(math.e) / math.sqrt(HEAD_SIZE)
START_MAX = -1e30
HIDDEN = -3e38


def attention_kernel(info, q_ref, span_ref, own_ref, other_ref, out_ref, acc_ref):
    plane, core = info[0], info[1]
    lane_in_pack = lax.broadcasted_iota(jnp.int32, (1, 2 * HEAD_SIZE), 1)
    is_value = lane_in_pack >= HEAD_SIZE

    def one_pair(pair, _):
        first_tile = info[2 + 3 * pair]
        last_lo = info[3 + 3 * pair]
        first_pos = info[4 + 3 * pair]
        last_tile = plane * Z + PAIR * pair + PAIR - 1
        pieces = []
        for b in range(PAIR):
            block = q_ref[PAIR * pair + b]
            for j in range(GROUP):
                pieces.append(block[:, j * HEAD_SIZE:(j + 1) * HEAD_SIZE])
        rows = jnp.concatenate(pieces, axis=0)
        rows = jnp.concatenate([rows, jnp.zeros_like(rows)], axis=1)
        lo = span_ref[pair, 0:1, :]
        hi = span_ref[pair, 1:2, :]
        acc_ref[...] = jnp.zeros_like(acc_ref)
        steps = lax.div(last_tile - first_tile + STEP_TILES, STEP_TILES)

        def attend(kv_ref, offset, top):
            def step(s, top):
                tile0 = first_tile + s * STEP_TILES
                parts = []
                for g in range(STEP_TILES):
                    tile = jnp.minimum(tile0 + g, X * Z - 1)
                    xi = lax.div(tile, Z)
                    zi = lax.rem(tile, Z)
                    for y in range(Y):
                        parts.append(kv_ref[xi * Y + y, zi])
                kv = jnp.concatenate(parts, axis=0)
                scores = lax.dot_general(kv, rows, (((1,), (1,)), ((), ())), preferred_element_type=jnp.float32)

                def finish(scores):
                    new_top = jnp.maximum(top, jnp.max(scores, axis=0, keepdims=True))
                    weights = jnp.exp2((scores - new_top) * EXP2_SCALE).astype(jnp.bfloat16)
                    shrink = jnp.exp2((top - new_top) * EXP2_SCALE)
                    ones_values = jnp.where(is_value, kv, jnp.ones_like(kv))
                    mixed = lax.dot_general(ones_values, weights, (((0,), (0,)), ((), ())), preferred_element_type=jnp.float32)
                    acc_ref[...] = acc_ref[...] * shrink + mixed
                    return new_top

                def masked(scores):
                    k = lax.broadcasted_iota(jnp.int32, (STEP_TILES * TILE, 1), 0)
                    pos = (tile0 + lax.div(k, TILE)) * (CORES * TILE) + offset * TILE + lax.rem(k, TILE)
                    return finish(jnp.where((pos >= lo) & (pos <= hi), scores, HIDDEN))

                begin = tile0 * (CORES * TILE) + offset * TILE
                end = (tile0 + STEP_TILES - 1) * (CORES * TILE) + offset * TILE + TILE - 1
                clear = (begin >= last_lo) & (end <= first_pos)
                return lax.cond(clear, finish, masked, scores)

            return lax.fori_loop(0, steps, step, top)

        top = jnp.full((1, ROWS), START_MAX, jnp.float32)
        top = attend(own_ref, core, top)
        top = attend(other_ref, 1 - core, top)
        total = acc_ref[0:1, :]
        result = (acc_ref[HEAD_SIZE:, :] / total).T
        for b in range(PAIR):
            heads = [
                result[(b * GROUP + j) * BLOCK:(b * GROUP + j + 1) * BLOCK] for j in range(GROUP)
            ]
            out_ref[PAIR * pair + b] = jnp.concatenate(heads, axis=1).astype(jnp.bfloat16)
        return 0

    lax.fori_loop(0, Z // PAIR, one_pair, 0)


def doc_start(positions, doc_bounds):
    starts = doc_bounds[:-1]
    return jnp.max(jnp.where(starts[None, :] <= positions[:, None], starts[None, :], 0), axis=1)


def on_device(queries, keys, values, doc_bounds):
    x, core, y = lax.axis_index("x"), lax.axis_index("core"), lax.axis_index("y")
    packed = jnp.concatenate(
        [keys.reshape(BLOCK, KEY_VALUE_HEADS, HEAD_SIZE), values.reshape(BLOCK, KEY_VALUE_HEADS, HEAD_SIZE)],
        axis=2,
    ).reshape(BLOCK, -1)
    packed = lax.all_to_all(packed, "z", split_axis=1, concat_axis=0, tiled=True)
    copies = jnp.broadcast_to(packed[None], (X * Y,) + packed.shape)
    own = lax.all_to_all(copies, ("x", "y"), split_axis=0, concat_axis=0, tiled=True)
    other = lax.ppermute(own, "core", [(0, 1), (1, 0)])
    own = own.reshape(X * Y, Z, BLOCK, 2 * HEAD_SIZE)
    other = other.reshape(X * Y, Z, BLOCK, 2 * HEAD_SIZE)
    q = lax.all_to_all(queries, "z", split_axis=1, concat_axis=0, tiled=True)
    q = q.reshape(Z, BLOCK, GROUP * HEAD_SIZE)

    base = x * (Z * CORES * TILE) + core * TILE + y * BLOCK
    pos = base + jnp.arange(Z, dtype=jnp.int32)[:, None] * (CORES * TILE) + jnp.arange(BLOCK, dtype=jnp.int32)[None, :]
    lo = doc_start(pos.reshape(-1), doc_bounds).reshape(Z, BLOCK)

    def as_rows(a):
        a = a.reshape(Z // PAIR, PAIR, 1, BLOCK)
        return jnp.broadcast_to(a, (Z // PAIR, PAIR, GROUP, BLOCK)).reshape(Z // PAIR, 1, ROWS)

    span = jnp.concatenate([as_rows(lo), as_rows(pos)], axis=1)
    per_pair = jnp.stack(
        [lo[::PAIR, 0] // (CORES * TILE), lo[PAIR - 1::PAIR, -1], pos[::PAIR, 0]], axis=1
    ).reshape(-1)
    info = jnp.concatenate([jnp.stack([x, core]).astype(jnp.int32), per_pair])
    attended = pl.pallas_call(
        attention_kernel,
        out_shape=jax.ShapeDtypeStruct((Z, BLOCK, GROUP * HEAD_SIZE), jnp.bfloat16),
        in_specs=[pl.BlockSpec(memory_space=pltpu.SMEM)] + [pl.BlockSpec(memory_space=pltpu.VMEM)] * 4,
        out_specs=pl.BlockSpec(memory_space=pltpu.VMEM),
        scratch_shapes=[pltpu.VMEM((2 * HEAD_SIZE, ROWS), jnp.float32)],
        compiler_params=pltpu.CompilerParams(vmem_limit_bytes=48 * 1024 * 1024),
        name="attention",
    )(info, q, span, own, other)
    attended = attended.reshape(Z * BLOCK, GROUP * HEAD_SIZE)
    return lax.all_to_all(attended, "z", split_axis=0, concat_axis=1, tiled=True)


def solution(mesh):
    split = Mesh(mesh.devices.reshape(X, Z, CORES, Y), ("x", "z", "core", "y"))
    rows = P(("x", "z", "core", "y"), None)
    return jax.shard_map(
        on_device,
        mesh=split,
        in_specs=(rows, rows, rows, P()),
        out_specs=rows,
        check_vma=False,
    )
```

```python
import functools
import math

import jax
import jax.numpy as jnp
from jax import lax
from jax.experimental import pallas as pl
from jax.experimental.pallas import tpu as pltpu
from jax.sharding import Mesh, PartitionSpec as P

QUERY_HEADS = 32
KEY_VALUE_HEADS = 8
HEAD_SIZE = 64
GROUP = QUERY_HEADS // KEY_VALUE_HEADS

X, Z, CORES, Y = 4, 8, 2, 4
BLOCK = 64
TILE = Y * BLOCK
SPAN = CORES * TILE
PAIR = 2
PAIRS = Z // PAIR
ROWS = PAIR * GROUP * BLOCK
KEYS = PAIR * TILE
WIDE = 2 * HEAD_SIZE

EXP2_SCALE = math.log2(math.e) / math.sqrt(HEAD_SIZE)
START_MAX = -1e30
HIDDEN = -3e38
LARGEST_SUM = 2.0 ** 60


def attention_kernel(stage, info, q_ref, span_ref, *refs):
    if stage == 0:
        own_ref, acc_ref, top_ref, rows_ref = refs
    else:
        own_ref, other_ref, acc_in, top_ref, rows_ref, out_ref, acc_ref, run_ref = refs
    plane, core = info[0], info[1]
    single, start = info[2], info[3]
    lane = lax.broadcasted_iota(jnp.int32, (KEYS, WIDE), 1)

    if stage == 0:
        filler = (lax.broadcasted_iota(jnp.int32, (HEAD_SIZE, ROWS), 0) == 0).astype(jnp.bfloat16)
        for p in range(PAIRS):
            pieces = []
            for b in range(PAIR):
                block = q_ref[PAIR * p + b][:, WIDE:].T
                pieces += [block[j * HEAD_SIZE:(j + 1) * HEAD_SIZE] for j in range(GROUP)]
            rows_ref[p] = jnp.concatenate([jnp.concatenate(pieces, axis=1), filler], axis=0)
    else:
        acc_ref[...] = acc_in[...]

    def load(kv_ref, offset, block):
        xi, zi = lax.div(block, Z // PAIR), lax.rem(block, Z // PAIR) * PAIR
        kv = jnp.concatenate([kv_ref[xi * Y + y, zi + g] for g in range(PAIR) for y in range(Y)], axis=0)
        k = lax.broadcasted_iota(jnp.int32, (KEYS, 1), 0)
        pos = block * (PAIR * SPAN) + offset * TILE + lax.div(k, TILE) * SPAN + lax.rem(k, TILE)
        bias = jnp.where(pos < start, START_MAX, 0.0)
        keys = jnp.where(lane == HEAD_SIZE, bias, kv.astype(jnp.float32)).astype(jnp.bfloat16)
        values = jnp.where(lane < HEAD_SIZE, 1.0, kv.astype(jnp.float32)).astype(jnp.bfloat16).T
        return keys, values, pos

    def scores_of(keys, p):
        return jnp.dot(keys, rows_ref[p], preferred_element_type=jnp.float32)

    def mix(values, weights):
        return jnp.dot(values, weights.astype(jnp.bfloat16), preferred_element_type=jnp.float32)

    def plain(kv_ref, offset, block, pairs, causal):
        keys, values, pos = load(kv_ref, offset, block)
        for p in pairs:
            scores = scores_of(keys, p)
            if causal:
                scores = jnp.where(pos <= span_ref[p, 1:2, :], scores, HIDDEN)
            weights = jnp.exp2(scores * EXP2_SCALE - top_ref[p] * EXP2_SCALE)
            acc_ref[p] += mix(values, weights)

    def fast(kv_ref, offset, own):
        begin = lax.div(start, PAIR * SPAN)
        home = plane * PAIRS
        for p in range(PAIRS):
            if own:
                keys, values, pos = load(kv_ref, offset, home + p)
                scores = jnp.where(pos <= span_ref[p, 1:2, :], scores_of(keys, p), HIDDEN)
                top = jnp.max(scores, axis=0, keepdims=True)
                top_ref[p] = top
                acc_ref[p] = mix(values, jnp.exp2(scores * EXP2_SCALE - top * EXP2_SCALE))
            else:
                plain(kv_ref, offset, home + p, [p], True)

        def step(block, _):
            plain(kv_ref, offset, block, list(range(PAIRS)), False)
            return 0

        lax.fori_loop(begin, home, step, 0)
        for b in range(PAIRS - 1):
            plain(kv_ref, offset, home + b, list(range(b + 1, PAIRS)), False)

    def online(kv_ref, offset, max_ref):
        def one(p, _):
            def step(block, _):
                keys, values, pos = load(kv_ref, offset, block)
                seen = (pos >= span_ref[p, 0:1, :]) & (pos <= span_ref[p, 1:2, :])
                scores = jnp.where(seen, scores_of(keys, p), HIDDEN)
                top = max_ref[p]
                new_top = jnp.maximum(top, jnp.max(scores, axis=0, keepdims=True))
                shrink = jnp.exp2((top - new_top) * EXP2_SCALE)
                acc_ref[p] = acc_ref[p] * shrink + mix(values, jnp.exp2((scores - new_top) * EXP2_SCALE))
                max_ref[p] = new_top
                return 0

            lax.fori_loop(lax.div(info[4 + p], PAIR * SPAN), plane * PAIRS + p + 1, step, 0)
            return 0

        lax.fori_loop(0, PAIRS, one, 0)

    def clear(max_ref):
        acc_ref[...] = jnp.zeros_like(acc_ref)
        max_ref[...] = jnp.full(max_ref.shape, START_MAX, jnp.float32)

    if stage == 0:
        @pl.when(single == 1)
        def _():
            fast(own_ref, core, True)

        @pl.when(single == 0)
        def _():
            clear(top_ref)
            online(own_ref, core, top_ref)
        return

    @pl.when(single == 1)
    def _():
        fast(other_ref, 1 - core, False)

    within = jnp.float32(1)
    for p in range(PAIRS):
        within = jnp.minimum(within, jnp.min((acc_ref[p, 0:1, :] <= LARGEST_SUM).astype(jnp.float32)))
    again = (single == 1) & (within < 0.5)

    @pl.when(again)
    def _():
        clear(run_ref)
        online(own_ref, core, run_ref)

    @pl.when(single == 0)
    def _():
        run_ref[...] = top_ref[...]

    @pl.when((single == 0) | again)
    def _():
        online(other_ref, 1 - core, run_ref)

    for p in range(PAIRS):
        result = (acc_ref[p, HEAD_SIZE:, :] / acc_ref[p, 0:1, :]).T
        for b in range(PAIR):
            heads = [result[(b * GROUP + j) * BLOCK:(b * GROUP + j + 1) * BLOCK] for j in range(GROUP)]
            out_ref[PAIR * p + b] = jnp.concatenate(heads, axis=1).astype(jnp.bfloat16)


def doc_start(positions, doc_bounds):
    starts = doc_bounds[:-1]
    return jnp.max(jnp.where(starts[None, :] <= positions[:, None], starts[None, :], 0), axis=1)


def on_device(queries, keys, values, doc_bounds):
    x, core, y = lax.axis_index("x"), lax.axis_index("core"), lax.axis_index("y")
    heads = (BLOCK, KEY_VALUE_HEADS, -1)
    packed = jnp.concatenate([keys.reshape(heads), values.reshape(heads), queries.reshape(heads)], axis=2)
    packed = lax.all_to_all(packed, "z", split_axis=1, concat_axis=0, tiled=True)
    packed = packed.reshape(Z, BLOCK, WIDE + GROUP * HEAD_SIZE)
    copies = jnp.broadcast_to(packed[None, :, :, :WIDE], (X * Y, Z, BLOCK, WIDE))
    own = lax.all_to_all(copies, ("x", "y"), split_axis=0, concat_axis=0, tiled=True)
    other = lax.ppermute(own, "core", [(0, 1), (1, 0)])

    base = x * (Z * SPAN) + core * TILE + y * BLOCK
    pos = base + jnp.arange(Z, dtype=jnp.int32)[:, None] * SPAN + jnp.arange(BLOCK, dtype=jnp.int32)[None, :]
    lo = doc_start(pos.reshape(-1), doc_bounds).reshape(Z, BLOCK)

    def as_rows(a):
        a = a.reshape(PAIRS, PAIR, 1, BLOCK)
        return jnp.broadcast_to(a, (PAIRS, PAIR, GROUP, BLOCK)).reshape(PAIRS, 1, ROWS)

    span = jnp.concatenate([as_rows(lo), as_rows(pos)], axis=1)
    head = jnp.stack([x, core, (lo[0, 0] == lo[-1, -1]).astype(jnp.int32), lo[0, 0]])
    info = jnp.concatenate([head.astype(jnp.int32), lo[::PAIR, 0]])
    smem = pl.BlockSpec(memory_space=pltpu.SMEM)
    vmem = pl.BlockSpec(memory_space=pltpu.VMEM)
    acc_shape = jax.ShapeDtypeStruct((PAIRS, WIDE, ROWS), jnp.float32)
    top_shape = jax.ShapeDtypeStruct((PAIRS, 1, ROWS), jnp.float32)
    rows_shape = jax.ShapeDtypeStruct((PAIRS, WIDE, ROWS), jnp.bfloat16)
    params = pltpu.CompilerParams(vmem_limit_bytes=40 * 1024 * 1024)
    acc, top, rows = pl.pallas_call(
        functools.partial(attention_kernel, 0),
        out_shape=(acc_shape, top_shape, rows_shape),
        in_specs=[smem] + [vmem] * 3,
        out_specs=(vmem,) * 3,
        compiler_params=params,
        name="attention_own",
    )(info, packed, span, own)
    attended = pl.pallas_call(
        functools.partial(attention_kernel, 1),
        out_shape=jax.ShapeDtypeStruct((Z, BLOCK, GROUP * HEAD_SIZE), jnp.bfloat16),
        in_specs=[smem] + [vmem] * 7,
        out_specs=vmem,
        scratch_shapes=[pltpu.VMEM(acc_shape.shape, jnp.float32), pltpu.VMEM(top_shape.shape, jnp.float32)],
        compiler_params=params,
        name="attention_other",
    )(info, packed, span, own, other, acc, top, rows)
    attended = attended.reshape(Z * BLOCK, GROUP * HEAD_SIZE)
    return lax.all_to_all(attended, "z", split_axis=0, concat_axis=1, tiled=True)


def solution(mesh):
    split = Mesh(mesh.devices.reshape(X, Z, CORES, Y), ("x", "z", "core", "y"))
    rows = P(("x", "z", "core", "y"), None)
    return jax.shard_map(
        on_device,
        mesh=split,
        in_specs=(rows, rows, rows, P()),
        out_specs=rows,
        check_vma=False,
    )
```

```python
import functools
import math

import jax
import jax.numpy as jnp
from jax import lax
from jax.experimental import pallas as pl
from jax.experimental.pallas import tpu as pltpu
from jax.sharding import Mesh, PartitionSpec as P

QUERY_HEADS = 32
KEY_VALUE_HEADS = 8
HEAD_SIZE = 64
DOCS = 16
GROUP = QUERY_HEADS // KEY_VALUE_HEADS

X, Z, CORES, Y = 4, 8, 2, 4
AXES = ("x", "z", "core", "y")
BLOCK = 64
TILE = Y * BLOCK
SPAN = CORES * TILE
PAIR = 2
PAIRS = Z // PAIR
PLANE = Z * SPAN
STRIDE = PAIR * SPAN
HALF = GROUP * BLOCK
ROWS = PAIR * HALF
KEYS = PAIR * TILE
WIDE = 2 * HEAD_SIZE
HEAD_COLS = GROUP * HEAD_SIZE
INNER = (2, 3, 4, 5)
SETS = ((0, 3), (1, 2))

EXP2_SCALE = math.log2(math.e) / math.sqrt(HEAD_SIZE)
START_MAX = -1e30
HIDDEN = -3e38
LARGEST_SUM = 2.0 ** 60


def twisted_groups():
    groups = []
    for a in range(X):
        for core in range(CORES):
            for y in range(Y):
                group = []
                for z in range(Z):
                    x = X - 1 - a if z in INNER else a
                    group.append(((x * Z + z) * CORES + core) * Y + y)
                groups.append(group)
    return groups


def is_inner(z):
    return (z >= INNER[0]) & (z <= INNER[-1])


def attention_kernel(stage, bounds, q_ref, *refs):
    if stage == 0:
        own_ref, acc_ref, top_ref, rows_ref = refs
    else:
        own_ref, other_ref, acc_in, top_ref, rows_ref, out_ref, acc_ref, run_ref = refs
    x, z, core, y = (lax.axis_index(a) for a in AXES)
    inner = is_inner(z)
    outer_plane = jnp.where(inner, X - 1 - x, x)
    planes = (outer_plane, X - 1 - outer_plane)
    column = lax.broadcasted_iota(jnp.int32, (1, WIDE), 1)
    key_lanes = (column < HEAD_SIZE).astype(jnp.bfloat16)
    value_lanes = (column >= HEAD_SIZE).astype(jnp.bfloat16)
    row = lax.broadcasted_iota(jnp.int32, (1, ROWS), 1)
    row_token = lax.rem(row, BLOCK)
    key = lax.broadcasted_iota(jnp.int32, (KEYS, 1), 0)
    key_tile = lax.div(key, TILE)
    key_y = lax.rem(y + lax.div(lax.rem(key, TILE), BLOCK), Y)
    key_token = lax.rem(key, BLOCK)

    def doc_start(position):
        start = jnp.int32(0)
        for d in range(1, DOCS):
            start = jnp.where(bounds[d] <= position, bounds[d], start)
        return start

    def token(plane, block, t):
        return plane * PLANE + block * SPAN + core * TILE + y * BLOCK + t

    starts, single = [], []
    for plane, pairs in zip(planes, SETS):
        start = doc_start(token(plane, PAIR * pairs[0], 0))
        starts.append(start)
        single.append(start == doc_start(token(plane, PAIR * pairs[1] + PAIR - 1, BLOCK - 1)))

    if stage == 0:
        line = lax.broadcasted_iota(jnp.int32, (HEAD_SIZE, ROWS), 0)
        half = lax.broadcasted_iota(jnp.int32, (HEAD_SIZE, ROWS), 1) // HALF
        filler = ((line == 0) | (line == half + 1)).astype(jnp.bfloat16)
        for p in range(PAIRS):
            pieces = []
            for b in range(PAIR):
                block = q_ref[PAIR * p + b][:, WIDE:].T
                pieces += [block[j * HEAD_SIZE:(j + 1) * HEAD_SIZE] for j in range(GROUP)]
            rows_ref[p] = jnp.concatenate([jnp.concatenate(pieces, axis=1), filler], axis=0)
    else:
        acc_ref[...] = acc_in[...]
        run_ref[...] = top_ref[...]

    def load(kv_ref, offset, block, start, diagonal=False):
        plane, zi = lax.div(block, PAIRS), lax.rem(block, PAIRS) * PAIR
        source = jnp.where(is_inner(zi) == inner, plane, X - 1 - plane)
        parts = []
        for g in range(PAIR):
            for i in range(Y):
                parts.append(kv_ref[source * Y + lax.rem(y + i, Y), zi + g])
        kv = jnp.concatenate(parts, axis=0)
        pos = block * STRIDE + key_tile * SPAN + offset * TILE + key_y * BLOCK + key_token
        bias = jnp.where((column == HEAD_SIZE) & (pos < start), START_MAX, 0.0)
        if diagonal:
            if offset is core:
                later = key_y > y
            else:
                later = jnp.broadcast_to(offset > core, key.shape)
            for b in range(PAIR):
                unseen = (key_tile > b) | ((key_tile == b) & later)
                bias = jnp.where((column == HEAD_SIZE + 1 + b) & unseen, START_MAX, bias)
        keys = kv * key_lanes + bias.astype(jnp.bfloat16)
        values = (kv * value_lanes + key_lanes).T
        return keys, values, pos

    def scores_of(keys, p):
        return jnp.dot(keys, rows_ref[p], preferred_element_type=jnp.float32)

    def mix(values, weights):
        return jnp.dot(values, weights.astype(jnp.bfloat16), preferred_element_type=jnp.float32)

    def plain(kv_ref, offset, block, start, pairs, diagonal=False):
        keys, values, _ = load(kv_ref, offset, block, start, diagonal)
        for p in pairs:
            weights = jnp.exp2(scores_of(keys, p) * EXP2_SCALE - top_ref[p] * EXP2_SCALE)
            acc_ref[p] += mix(values, weights)

    def first(kv_ref, block, start, p):
        keys, values, _ = load(kv_ref, core, block, start, True)
        scores = scores_of(keys, p)
        parts = []
        for b in range(PAIR):
            at = b * TILE
            t = lax.broadcasted_iota(jnp.int32, (BLOCK, 1), 0)
            hidden = (t > row_token) & (row // HALF == b)
            parts += [jnp.where(hidden, HIDDEN, scores[at:at + BLOCK]), scores[at + BLOCK:at + TILE]]
        scores = jnp.concatenate(parts, axis=0)
        top = jnp.max(scores, axis=0, keepdims=True)
        top_ref[p] = top
        acc_ref[p] = mix(values, jnp.exp2(scores * EXP2_SCALE - top * EXP2_SCALE))

    def fast(kv_ref, offset, s):
        start, home = starts[s], planes[s] * PAIRS
        low, high = SETS[s]
        for p in (low, high):
            if stage == 0:
                first(kv_ref, home + p, start, p)
            else:
                plain(kv_ref, offset, home + p, start, [p], True)
        for b in range(low, high):
            plain(kv_ref, offset, home + b, start, [high])

        def step(block, _):
            plain(kv_ref, offset, block, start, [low, high])
            return 0

        lax.fori_loop(lax.div(start, STRIDE), home + low, step, 0)

    def online(kv_ref, offset, max_ref, s):
        plane = planes[s]

        def one(i, _):
            p = SETS[s][0] + i * (SETS[s][1] - SETS[s][0])
            begin = doc_start(token(plane, PAIR * p, 0))
            hi = token(plane, PAIR * p + row // HALF, row_token)
            lo = doc_start(hi)

            def step(block, _):
                keys, values, pos = load(kv_ref, offset, block, begin)
                scores = jnp.where((pos >= lo) & (pos <= hi), scores_of(keys, p), HIDDEN)
                top = max_ref[p]
                new_top = jnp.maximum(top, jnp.max(scores, axis=0, keepdims=True))
                shrink = jnp.exp2((top - new_top) * EXP2_SCALE)
                acc_ref[p] = acc_ref[p] * shrink + mix(values, jnp.exp2((scores - new_top) * EXP2_SCALE))
                max_ref[p] = new_top
                return 0

            lax.fori_loop(lax.div(begin, STRIDE), plane * PAIRS + p + 1, step, 0)
            return 0

        lax.fori_loop(0, len(SETS[s]), one, 0)

    def clear(max_ref, s):
        for p in SETS[s]:
            acc_ref[p] = jnp.zeros((WIDE, ROWS), jnp.float32)
            max_ref[p] = jnp.full((1, ROWS), START_MAX, jnp.float32)

    for s in range(len(SETS)):
        if stage == 0:
            @pl.when(single[s])
            def _():
                fast(own_ref, core, s)

            @pl.when(jnp.logical_not(single[s]))
            def _():
                clear(top_ref, s)
                online(own_ref, core, top_ref, s)
        else:
            @pl.when(single[s])
            def _():
                fast(other_ref, 1 - core, s)

            within = jnp.float32(1)
            for p in SETS[s]:
                within = jnp.minimum(within, jnp.min((acc_ref[p, 0:1, :] <= LARGEST_SUM).astype(jnp.float32)))
            again = single[s] & (within < 0.5)

            @pl.when(again)
            def _():
                clear(run_ref, s)
                online(own_ref, core, run_ref, s)

            @pl.when(jnp.logical_not(single[s]) | again)
            def _():
                online(other_ref, 1 - core, run_ref, s)

    if stage == 0:
        return
    for p in range(PAIRS):
        result = (acc_ref[p, HEAD_SIZE:, :] / acc_ref[p, 0:1, :]).T
        for b in range(PAIR):
            heads = [result[(b * GROUP + j) * BLOCK:(b * GROUP + j + 1) * BLOCK] for j in range(GROUP)]
            out_ref[PAIR * p + b] = jnp.concatenate(heads, axis=1).astype(jnp.bfloat16)


def pack_kernel(q_ref, k_ref, v_ref, out_ref):
    for h in range(KEY_VALUE_HEADS):
        cols = slice(h * HEAD_SIZE, (h + 1) * HEAD_SIZE)
        out_ref[h, :, :WIDE] = jnp.concatenate([k_ref[:, cols], v_ref[:, cols]], axis=1)
        out_ref[h, :, WIDE:] = q_ref[:, h * HEAD_COLS:(h + 1) * HEAD_COLS]


def on_device(queries, keys, values, doc_bounds):
    smem = pl.BlockSpec(memory_space=pltpu.SMEM)
    vmem = pl.BlockSpec(memory_space=pltpu.VMEM)
    groups = twisted_groups()
    packed = pl.pallas_call(
        pack_kernel,
        out_shape=jax.ShapeDtypeStruct((Z, BLOCK, WIDE + HEAD_COLS), jnp.bfloat16),
        in_specs=[vmem] * 3,
        out_specs=vmem,
        name="pack",
    )(queries, keys, values)
    packed = lax.all_to_all(packed, AXES, 0, 0, axis_index_groups=groups, tiled=True)
    copies = jnp.broadcast_to(packed[None, :, :, :WIDE], (X * Y, Z, BLOCK, WIDE))
    own = lax.all_to_all(copies, ("x", "y"), 0, 0, tiled=True)
    other = lax.ppermute(own, "core", [(0, 1), (1, 0)])

    acc_shape = jax.ShapeDtypeStruct((PAIRS, WIDE, ROWS), jnp.float32)
    top_shape = jax.ShapeDtypeStruct((PAIRS, 1, ROWS), jnp.float32)
    rows_shape = jax.ShapeDtypeStruct((PAIRS, WIDE, ROWS), jnp.bfloat16)
    params = pltpu.CompilerParams(vmem_limit_bytes=40 * 1024 * 1024)
    acc, top, rows = pl.pallas_call(
        functools.partial(attention_kernel, 0),
        out_shape=(acc_shape, top_shape, rows_shape),
        in_specs=[smem] + [vmem] * 2,
        out_specs=(vmem,) * 3,
        compiler_params=params,
        name="attention_own",
    )(doc_bounds, packed, own)
    attended = pl.pallas_call(
        functools.partial(attention_kernel, 1),
        out_shape=jax.ShapeDtypeStruct((Z, BLOCK, HEAD_COLS), jnp.bfloat16),
        in_specs=[smem] + [vmem] * 6,
        out_specs=vmem,
        scratch_shapes=[pltpu.VMEM(acc_shape.shape, jnp.float32), pltpu.VMEM(top_shape.shape, jnp.float32)],
        compiler_params=params,
        name="attention_other",
    )(doc_bounds, packed, own, other, acc, top, rows)
    attended = lax.all_to_all(attended, AXES, 0, 0, axis_index_groups=groups, tiled=True)
    return attended.transpose(1, 0, 2).reshape(BLOCK, QUERY_HEADS * HEAD_SIZE)


def solution(mesh):
    split = Mesh(mesh.devices.reshape(X, Z, CORES, Y), AXES)
    rows = P(AXES, None)
    return jax.shard_map(
        on_device,
        mesh=split,
        in_specs=(rows, rows, rows, P()),
        out_specs=rows,
        check_vma=False,
    )
```

```python
import functools
import math

import jax
import jax.numpy as jnp
from jax import lax
from jax.experimental import pallas as pl
from jax.experimental.pallas import tpu as pltpu
from jax.sharding import Mesh, PartitionSpec as P


QUERY_HEADS = 32
KEY_VALUE_HEADS = 8
HEAD_SIZE = 64
DOCS = 16
GROUP = QUERY_HEADS // KEY_VALUE_HEADS

X, Z, CORES, Y = 4, 8, 2, 4
AXES = ("x", "z", "core", "y")
BLOCK = 64
TILE = Y * BLOCK
SPAN = CORES * TILE
PAIR = 2
PAIRS = Z // PAIR
PLANE = Z * SPAN
STRIDE = PAIR * SPAN
HALF = GROUP * BLOCK
ROWS = PAIR * HALF
KEYS = PAIR * TILE
WIDE = 2 * HEAD_SIZE
HEAD_COLS = GROUP * HEAD_SIZE
INNER = (2, 3, 4, 5)
SETS = ((0, 3), (1, 2))

EXP2_SCALE = math.log2(math.e) / math.sqrt(HEAD_SIZE)
START_MAX = -1e30
HIDDEN = -3e38
LARGEST_SUM = 2.0 ** 60


def twisted_groups():
    groups = []
    for a in range(X):
        for core in range(CORES):
            for y in range(Y):
                group = []
                for z in range(Z):
                    x = X - 1 - a if z in INNER else a
                    group.append(((x * Z + z) * CORES + core) * Y + y)
                groups.append(group)
    return groups


def is_inner(z):
    return (z >= INNER[0]) & (z <= INNER[-1])


def line_groups(first):
    index = lambda x, z, core, y: ((x * Z + z) * CORES + core) * Y + y
    groups = []
    for z in range(Z):
        for core in range(CORES):
            if (core == 0) == first:
                groups += [[index(x, z, core, y) for x in range(X)] for y in range(Y)]
            else:
                groups += [[index(x, z, core, y) for y in range(Y)] for x in range(X)]
    return groups


def place():
    x, z, core, y = (lax.axis_index(a) for a in AXES)
    inner = is_inner(z)
    outer_plane = jnp.where(inner, X - 1 - x, x)
    return inner, core, y, (outer_plane, X - 1 - outer_plane)


def doc_start(bounds, position):
    start = jnp.zeros_like(position)
    for d in range(1, DOCS):
        start = jnp.where(bounds[d] <= position, bounds[d], start)
    return start


def lanes():
    column = lax.broadcasted_iota(jnp.int32, (1, WIDE), 1)
    return column, (column < HEAD_SIZE).astype(jnp.bfloat16), (column >= HEAD_SIZE).astype(jnp.bfloat16)


def mix(values, weights):
    return jnp.dot(values, weights.astype(jnp.bfloat16), preferred_element_type=jnp.float32)


def start_kernel(bounds, q_ref, rows_ref, top_ref, acc_ref):
    _, core, y, planes = place()
    _, key_lanes, value_lanes = lanes()
    line = lax.broadcasted_iota(jnp.int32, (HEAD_SIZE, ROWS), 0)
    half = lax.broadcasted_iota(jnp.int32, (HEAD_SIZE, ROWS), 1) // HALF
    filler = ((line == 0) | (line == half + 1)).astype(jnp.bfloat16)
    row = lax.broadcasted_iota(jnp.int32, (1, ROWS), 1)
    key = lax.broadcasted_iota(jnp.int32, (PAIR * BLOCK, 1), 0)
    for plane, pairs in zip(planes, SETS):
        for p in pairs:
            pieces = []
            for b in range(PAIR):
                block = q_ref[PAIR * p + b][:, WIDE:].T
                pieces += [block[j * HEAD_SIZE:(j + 1) * HEAD_SIZE] for j in range(GROUP)]
            rows = jnp.concatenate([jnp.concatenate(pieces, axis=1), filler], axis=0)
            rows_ref[p] = rows
            kv = jnp.concatenate([q_ref[PAIR * p + b][:, :WIDE] for b in range(PAIR)], axis=0)
            base = plane * PLANE + PAIR * p * SPAN + core * TILE + y * BLOCK
            pos = base + lax.div(key, BLOCK) * SPAN + lax.rem(key, BLOCK)
            hi = base + row // HALF * SPAN + lax.rem(row, BLOCK)
            scores = jnp.dot(kv * key_lanes, rows, preferred_element_type=jnp.float32)
            scores = jnp.where((pos >= doc_start(bounds, hi)) & (pos <= hi), scores, HIDDEN)
            top = jnp.max(scores, axis=0, keepdims=True)
            top_ref[p] = top
            values = (kv * value_lanes + key_lanes).T
            acc_ref[p] = mix(values, jnp.exp2(scores * EXP2_SCALE - top * EXP2_SCALE))


def attention_kernel(stage, bounds, rows_ref, top_ref, acc_in, *refs):
    if stage == 0:
        own_ref, acc_ref = refs
    else:
        own_ref, other_ref, out_ref, acc_ref, run_ref = refs
    inner, core, y, planes = place()
    column, key_lanes, value_lanes = lanes()
    row = lax.broadcasted_iota(jnp.int32, (1, ROWS), 1)
    row_token = lax.rem(row, BLOCK)
    key = lax.broadcasted_iota(jnp.int32, (KEYS, 1), 0)
    key_tile = lax.div(key, TILE)
    key_y = lax.div(lax.rem(key, TILE), BLOCK)
    key_token = lax.rem(key, BLOCK)
    acc_ref[...] = acc_in[...]

    def token(plane, block, t):
        return plane * PLANE + block * SPAN + core * TILE + y * BLOCK + t

    starts, single = [], []
    for plane, pairs in zip(planes, SETS):
        start = doc_start(bounds, token(plane, PAIR * pairs[0], 0))
        starts.append(start)
        single.append(start == doc_start(bounds, token(plane, PAIR * pairs[1] + PAIR - 1, BLOCK - 1)))

    def load(kv_ref, offset, block, start, diagonal=False):
        plane, zi = lax.div(block, PAIRS), lax.rem(block, PAIRS) * PAIR
        source = jnp.where(is_inner(zi) == inner, plane, X - 1 - plane)
        parts = []
        for g in range(PAIR):
            for i in range(Y):
                at = jnp.where(offset == 0, i * X + source, source * Y + i)
                parts.append(kv_ref[at, zi + g])
        kv = jnp.concatenate(parts, axis=0)
        pos = block * STRIDE + key_tile * SPAN + offset * TILE + key_y * BLOCK + key_token
        bias = jnp.where((column == HEAD_SIZE) & (pos < start), START_MAX, 0.0)
        if diagonal:
            for b in range(PAIR):
                if offset is core:
                    unseen = ((key_tile == b) & (key_y > y)) | (key_y == y)
                else:
                    unseen = (key_tile == b) & (offset > core)
                unseen = unseen | (key_tile > b)
                bias = jnp.where((column == HEAD_SIZE + 1 + b) & unseen, START_MAX, bias)
        keys = kv * key_lanes + bias.astype(jnp.bfloat16)
        values = (kv * value_lanes + key_lanes).T
        return keys, values, pos

    def scores_of(keys, p):
        return jnp.dot(keys, rows_ref[p], preferred_element_type=jnp.float32)

    def plain(kv_ref, offset, block, start, pairs, diagonal=False, lo=None):
        keys, values, pos = load(kv_ref, offset, block, start, diagonal)
        for p in pairs:
            scores = scores_of(keys, p)
            if lo is not None:
                scores = jnp.where(pos >= lo, scores, HIDDEN)
            weights = jnp.exp2(scores * EXP2_SCALE - top_ref[p] * EXP2_SCALE)
            acc_ref[p] += mix(values, weights)

    def one_document(kv_ref, offset, s):
        start, home = starts[s], planes[s] * PAIRS
        low, high = SETS[s]
        for p in (low, high):
            plain(kv_ref, offset, home + p, start, [p], True)
        for b in range(low, high):
            plain(kv_ref, offset, home + b, start, [high])

        def step(block, _):
            plain(kv_ref, offset, block, start, [low, high])
            return 0

        lax.fori_loop(lax.div(start, STRIDE), home + low, step, 0)

    def row_limits(plane, p):
        hi = token(plane, PAIR * p + row // HALF, row_token)
        return doc_start(bounds, token(plane, PAIR * p, 0)), doc_start(bounds, hi), hi

    def documents(kv_ref, offset, s):
        plane = planes[s]
        for p in SETS[s]:
            begin, lo, _ = row_limits(plane, p)
            home = plane * PAIRS + p

            def step(block, _):
                plain(kv_ref, offset, block, begin, [p], False, lo)
                return 0

            lax.fori_loop(lax.div(begin, STRIDE), home, step, 0)
            plain(kv_ref, offset, home, begin, [p], True, lo)

    def online(kv_ref, offset, s):
        plane = planes[s]

        def one(i, _):
            p = SETS[s][0] + i * (SETS[s][1] - SETS[s][0])
            begin, lo, hi = row_limits(plane, p)

            def step(block, _):
                keys, values, pos = load(kv_ref, offset, block, begin)
                scores = jnp.where((pos >= lo) & (pos <= hi), scores_of(keys, p), HIDDEN)
                top = run_ref[p]
                new_top = jnp.maximum(top, jnp.max(scores, axis=0, keepdims=True))
                shrink = jnp.exp2((top - new_top) * EXP2_SCALE)
                acc_ref[p] = acc_ref[p] * shrink + mix(values, jnp.exp2((scores - new_top) * EXP2_SCALE))
                run_ref[p] = new_top
                return 0

            lax.fori_loop(lax.div(begin, STRIDE), plane * PAIRS + p + 1, step, 0)
            return 0

        lax.fori_loop(0, len(SETS[s]), one, 0)

    for s in range(len(SETS)):
        kv_ref, offset = (own_ref, core) if stage == 0 else (other_ref, 1 - core)

        @pl.when(single[s])
        def _():
            one_document(kv_ref, offset, s)

        @pl.when(jnp.logical_not(single[s]))
        def _():
            documents(kv_ref, offset, s)

    if stage == 0:
        return
    for s in range(len(SETS)):
        within = jnp.float32(1)
        for p in SETS[s]:
            within = jnp.minimum(within, jnp.min((acc_ref[p, 0:1, :] <= LARGEST_SUM).astype(jnp.float32)))

        @pl.when(within < 0.5)
        def _():
            for p in SETS[s]:
                acc_ref[p] = jnp.zeros((WIDE, ROWS), jnp.float32)
                run_ref[p] = jnp.full((1, ROWS), START_MAX, jnp.float32)
            online(own_ref, core, s)
            online(other_ref, 1 - core, s)

    for p in range(PAIRS):
        result = (acc_ref[p, HEAD_SIZE:, :] / acc_ref[p, 0:1, :]).T
        for b in range(PAIR):
            heads = [result[(b * GROUP + j) * BLOCK:(b * GROUP + j + 1) * BLOCK] for j in range(GROUP)]
            out_ref[PAIR * p + b] = jnp.concatenate(heads, axis=1).astype(jnp.bfloat16)


def pack_kernel(q_ref, k_ref, v_ref, out_ref):
    for h in range(KEY_VALUE_HEADS):
        cols = slice(h * HEAD_SIZE, (h + 1) * HEAD_SIZE)
        out_ref[h, :, :WIDE] = jnp.concatenate([k_ref[:, cols], v_ref[:, cols]], axis=1)
        out_ref[h, :, WIDE:] = q_ref[:, h * HEAD_COLS:(h + 1) * HEAD_COLS]


def on_device(queries, keys, values, doc_bounds):
    smem = pl.BlockSpec(memory_space=pltpu.SMEM)
    vmem = pl.BlockSpec(memory_space=pltpu.VMEM)
    groups = twisted_groups()
    packed = pl.pallas_call(
        pack_kernel,
        out_shape=jax.ShapeDtypeStruct((Z, BLOCK, WIDE + HEAD_COLS), jnp.bfloat16),
        in_specs=[vmem] * 3,
        out_specs=vmem,
        name="pack",
    )(queries, keys, values)
    packed = lax.all_to_all(packed, AXES, 0, 0, axis_index_groups=groups, tiled=True)
    gathered = packed[:, :, :WIDE]
    for first in (True, False):
        copies = jnp.broadcast_to(gathered[None], (X,) + gathered.shape)
        gathered = lax.all_to_all(copies, AXES, 0, 0, axis_index_groups=line_groups(first), tiled=True)
    own = gathered.reshape(X * Y, Z, BLOCK, WIDE)
    other = lax.ppermute(own, "core", [(0, 1), (1, 0)])

    acc_shape = jax.ShapeDtypeStruct((PAIRS, WIDE, ROWS), jnp.float32)
    top_shape = jax.ShapeDtypeStruct((PAIRS, 1, ROWS), jnp.float32)
    rows_shape = jax.ShapeDtypeStruct((PAIRS, WIDE, ROWS), jnp.bfloat16)
    params = pltpu.CompilerParams(vmem_limit_bytes=40 * 1024 * 1024)
    rows, top, acc = pl.pallas_call(
        start_kernel,
        out_shape=(rows_shape, top_shape, acc_shape),
        in_specs=[smem, vmem],
        out_specs=(vmem,) * 3,
        compiler_params=params,
        name="attention_start",
    )(doc_bounds, packed)
    acc = pl.pallas_call(
        functools.partial(attention_kernel, 0),
        out_shape=acc_shape,
        in_specs=[smem] + [vmem] * 4,
        out_specs=vmem,
        compiler_params=params,
        name="attention_own",
    )(doc_bounds, rows, top, acc, own)
    attended = pl.pallas_call(
        functools.partial(attention_kernel, 1),
        out_shape=jax.ShapeDtypeStruct((Z, BLOCK, HEAD_COLS), jnp.bfloat16),
        in_specs=[smem] + [vmem] * 5,
        out_specs=vmem,
        scratch_shapes=[pltpu.VMEM(acc_shape.shape, jnp.float32), pltpu.VMEM(top_shape.shape, jnp.float32)],
        compiler_params=params,
        name="attention_other",
    )(doc_bounds, rows, top, acc, own, other)
    attended = lax.all_to_all(attended, AXES, 0, 0, axis_index_groups=groups, tiled=True)
    return attended.transpose(1, 0, 2).reshape(BLOCK, QUERY_HEADS * HEAD_SIZE)


def solution(mesh):
    split = Mesh(mesh.devices.reshape(X, Z, CORES, Y), AXES)
    rows = P(AXES, None)
    return jax.shard_map(
        on_device,
        mesh=split,
        in_specs=(rows, rows, rows, P()),
        out_specs=rows,
        check_vma=False,
    )
```

```python
import functools
import math

import jax
import jax.numpy as jnp
from jax import lax
from jax.experimental import pallas as pl
from jax.experimental.pallas import tpu as pltpu
from jax.sharding import Mesh, PartitionSpec as P

QUERY_HEADS = 32
KEY_VALUE_HEADS = 8
HEAD_SIZE = 64
DOCS = 16
GROUP = QUERY_HEADS // KEY_VALUE_HEADS

X, Z, CORES, Y = 4, 8, 2, 4
AXES = ("x", "z", "core", "y")
BLOCK = 64
TILE = Y * BLOCK
SPAN = CORES * TILE
PAIR = 2
PAIRS = Z // PAIR
PLANE = Z * SPAN
STRIDE = PAIR * SPAN
HALF = GROUP * BLOCK
ROWS = PAIR * HALF
KEYS = PAIR * TILE
WIDE = 2 * HEAD_SIZE
HEAD_COLS = GROUP * HEAD_SIZE
BASE = (3, 1, 0, 2)
BLOCKS = X * PAIRS
NEVER = 1 << 20

EXP2_SCALE = math.log2(math.e) / math.sqrt(HEAD_SIZE)
START_MAX = -1e30
HIDDEN = -3e38
LARGEST_SUM = 2.0 ** 60


def square_groups():
    groups = []
    for k in range(X):
        for core in range(CORES):
            for y in range(Y):
                groups.append([(((BASE[z // PAIR] ^ k) * Z + z) * CORES + core) * Y + y for z in range(Z)])
    return groups


def base_of(pair):
    base = jnp.int32(BASE[-1])
    for p in range(PAIRS - 1):
        base = jnp.where(pair == p, BASE[p], base)
    return base


def line_groups(first):
    index = lambda x, z, core, y: ((x * Z + z) * CORES + core) * Y + y
    groups = []
    for z in range(Z):
        for core in range(CORES):
            if (core == 0) == first:
                groups += [[index(x, z, core, y) for x in range(X)] for y in range(Y)]
            else:
                groups += [[index(x, z, core, y) for y in range(Y)] for x in range(X)]
    return groups


def doc_start(bounds, position):
    start = jnp.zeros_like(position)
    for d in range(1, DOCS):
        start = jnp.where(bounds[d] <= position, bounds[d], start)
    return start


def mix(values, weights):
    return jnp.dot(values, weights.astype(jnp.bfloat16), preferred_element_type=jnp.float32)


def attention_kernel(stage, bounds, *refs):
    if stage == 0:
        q_ref, own_ref, rows_ref, top_ref, acc_out = refs
    else:
        rows_ref, top_ref, acc_in, own_ref, other_ref, out_ref, acc_ref, run_ref = refs
    x, z, core, y = (lax.axis_index(a) for a in AXES)
    mine = base_of(lax.div(z, PAIR))
    group = x ^ mine
    column = lax.broadcasted_iota(jnp.int32, (1, WIDE), 1)
    key_lanes = (column < HEAD_SIZE).astype(jnp.bfloat16)
    value_lanes = (column >= HEAD_SIZE).astype(jnp.bfloat16)
    row = lax.broadcasted_iota(jnp.int32, (1, ROWS), 1)
    row_offset = lax.div(row, HALF) * SPAN + lax.rem(row, BLOCK)
    key = lax.broadcasted_iota(jnp.int32, (KEYS, WIDE), 0)
    key_offset = lax.div(key, TILE) * SPAN + lax.rem(key, TILE)
    kv_ref, offset = (own_ref, core) if stage == 0 else (other_ref, 1 - core)

    def one_pair(p, _):
        plane = base_of(p) ^ group
        home = plane * PAIRS + p
        first = home * STRIDE + core * TILE + y * BLOCK
        start = doc_start(bounds, first)
        begin = lax.div(start, STRIDE)
        one_document = start == doc_start(bounds, first + SPAN + BLOCK - 1)

        after = jnp.where(column == HEAD_SIZE + 1, first, jnp.where(column == HEAD_SIZE + 2, first + SPAN, NEVER))
        held = jnp.where(column == HEAD_SIZE, first, NEVER)

        def load(kv_ref, offset, blocks, limits=None):
            parts, masks, origins = [], [], []
            for n, block in enumerate(blocks):
                near = jnp.minimum(block, BLOCKS - 1)
                q = lax.rem(near, PAIRS)
                source = lax.div(near, PAIRS) ^ base_of(q) ^ mine
                for g in range(PAIR):
                    for i in range(Y):
                        at = jnp.where(offset == 0, i * X + source, source * Y + i)
                        parts.append(kv_ref[at, q * PAIR + g])
                origin = block * STRIDE + offset * TILE
                origins.append(origin)
                if limits is not None:
                    before = jnp.where(column == HEAD_SIZE, limits[n] - origin, -NEVER)
                    unseen = (key_offset < before) | (key_offset >= after - origin)
                    if stage == 0:
                        unseen = unseen | ((key_offset >= held - origin) & (key_offset < held + BLOCK - origin))
                    masks.append(jnp.where(unseen, START_MAX, 0.0))
            kv = jnp.concatenate(parts, axis=0)
            keys = kv * key_lanes
            if limits is not None:
                keys = keys + jnp.concatenate(masks, axis=0).astype(jnp.bfloat16)
            return keys, (kv * value_lanes + key_lanes).T, origins

        def across(origins, low, high=None):
            offsets = jnp.concatenate([key_offset] * (ROWS // WIDE), axis=1)
            seen = []
            for origin in origins:
                inside = offsets >= low - origin
                seen.append(inside if high is None else inside & (offsets <= high - origin))
            return seen

        def hide(scores, seen):
            parts = [jnp.where(m, scores[n * KEYS:(n + 1) * KEYS], HIDDEN) for n, m in enumerate(seen)]
            return jnp.concatenate(parts, axis=0)

        if stage == 0:
            line = lax.broadcasted_iota(jnp.int32, (HEAD_SIZE, ROWS), 0)
            half = lax.broadcasted_iota(jnp.int32, (HEAD_SIZE, ROWS), 1) // HALF
            filler = ((line == 0) | (line == half + 1)).astype(jnp.bfloat16)
            own = [q_ref[PAIR * p + b] for b in range(PAIR)]
            pieces = []
            for block in own:
                turned = block[:, WIDE:].T
                pieces += [turned[j * HEAD_SIZE:(j + 1) * HEAD_SIZE] for j in range(GROUP)]
            rows = jnp.concatenate([jnp.concatenate(pieces, axis=1), filler], axis=0)
            rows_ref[p] = rows
            kv = jnp.concatenate([block[:, :WIDE] for block in own], axis=0)
            k = lax.broadcasted_iota(jnp.int32, (PAIR * BLOCK, 1), 0)
            k_offset = lax.div(k, BLOCK) * SPAN + lax.rem(k, BLOCK)
            scores = jnp.dot(kv * key_lanes, rows, preferred_element_type=jnp.float32)
            lo = doc_start(bounds, first + row_offset) - first
            scores = jnp.where((k_offset >= lo) & (k_offset <= row_offset), scores, HIDDEN)
            top = jnp.max(scores, axis=0, keepdims=True)
            top_ref[p] = top
            acc = acc_out.at[p]
            acc[...] = mix((kv * value_lanes + key_lanes).T, jnp.exp2(scores * EXP2_SCALE - top * EXP2_SCALE))
        else:
            acc = acc_ref
            acc[...] = acc_in[p]

        def add(blocks, limits=None, lo=None):
            keys, values, origins = load(kv_ref, offset, blocks, limits)
            scores = jnp.dot(keys, rows_ref[p], preferred_element_type=jnp.float32)
            if lo is not None:
                scores = hide(scores, across(origins, lo))
            weights = jnp.exp2(scores * EXP2_SCALE - top_ref[p] * EXP2_SCALE)
            acc[...] += mix(values, weights)

        @pl.when(one_document)
        def _():
            add([home, begin], [start, jnp.where(begin == home, NEVER, start)])
            inside = home - begin - 1

            def step(s, _):
                add([begin + 1 + 2 * s, begin + 2 + 2 * s])
                return 0

            lax.fori_loop(0, lax.div(inside, 2), step, 0)

            @pl.when((inside > 0) & (lax.rem(inside, 2) == 1))
            def _():
                add([home - 1])

        @pl.when(jnp.logical_not(one_document))
        def _():
            lo = doc_start(bounds, first + row_offset)

            def step(s, _):
                add([begin + 2 * s, begin + 2 * s + 1], [start, start], lo)
                return 0

            lax.fori_loop(0, lax.div(home - begin + 2, 2), step, 0)

        if stage == 0:
            return 0

        within = jnp.min((acc[0:1, :] <= LARGEST_SUM).astype(jnp.float32))

        @pl.when(within < 0.5)
        def _():
            hi = first + row_offset
            lo = doc_start(bounds, hi)
            acc[...] = jnp.zeros_like(acc)
            run_ref[...] = jnp.full(run_ref.shape, START_MAX, jnp.float32)
            for again_ref, again_offset in ((own_ref, core), (other_ref, 1 - core)):
                def step(block, _):
                    keys, values, origins = load(again_ref, again_offset, [block])
                    scores = jnp.dot(keys, rows_ref[p], preferred_element_type=jnp.float32)
                    scores = hide(scores, across(origins, lo, hi))
                    top = run_ref[...]
                    new_top = jnp.maximum(top, jnp.max(scores, axis=0, keepdims=True))
                    shrink = jnp.exp2((top - new_top) * EXP2_SCALE)
                    acc[...] = acc[...] * shrink + mix(values, jnp.exp2((scores - new_top) * EXP2_SCALE))
                    run_ref[...] = new_top
                    return 0

                lax.fori_loop(begin, home + 1, step, 0)

        result = (acc[HEAD_SIZE:, :] / acc[0:1, :]).T
        for b in range(PAIR):
            heads = [result[(b * GROUP + j) * BLOCK:(b * GROUP + j + 1) * BLOCK] for j in range(GROUP)]
            out_ref[PAIR * p + b] = jnp.concatenate(heads, axis=1).astype(jnp.bfloat16)
        return 0

    lax.fori_loop(0, PAIRS, one_pair, 0)


def pack_kernel(q_ref, k_ref, v_ref, out_ref):
    for h in range(KEY_VALUE_HEADS):
        cols = slice(h * HEAD_SIZE, (h + 1) * HEAD_SIZE)
        out_ref[h, :, :WIDE] = jnp.concatenate([k_ref[:, cols], v_ref[:, cols]], axis=1)
        out_ref[h, :, WIDE:] = q_ref[:, h * HEAD_COLS:(h + 1) * HEAD_COLS]


def on_device(queries, keys, values, doc_bounds):
    smem = pl.BlockSpec(memory_space=pltpu.SMEM)
    vmem = pl.BlockSpec(memory_space=pltpu.VMEM)
    groups = square_groups()
    packed = pl.pallas_call(
        pack_kernel,
        out_shape=jax.ShapeDtypeStruct((Z, BLOCK, WIDE + HEAD_COLS), jnp.bfloat16),
        in_specs=[vmem] * 3,
        out_specs=vmem,
        name="pack",
    )(queries, keys, values)
    packed = lax.all_to_all(packed, AXES, 0, 0, axis_index_groups=groups, tiled=True)
    gathered = packed[:, :, :WIDE]
    for first in (True, False):
        copies = jnp.broadcast_to(gathered[None], (X,) + gathered.shape)
        gathered = lax.all_to_all(copies, AXES, 0, 0, axis_index_groups=line_groups(first), tiled=True)
    own = gathered.reshape(X * Y, Z, BLOCK, WIDE)
    other = lax.ppermute(own, "core", [(0, 1), (1, 0)])

    acc_shape = jax.ShapeDtypeStruct((PAIRS, WIDE, ROWS), jnp.float32)
    top_shape = jax.ShapeDtypeStruct((PAIRS, 1, ROWS), jnp.float32)
    rows_shape = jax.ShapeDtypeStruct((PAIRS, WIDE, ROWS), jnp.bfloat16)
    params = pltpu.CompilerParams(vmem_limit_bytes=40 * 1024 * 1024)
    rows, top, acc = pl.pallas_call(
        functools.partial(attention_kernel, 0),
        out_shape=(rows_shape, top_shape, acc_shape),
        in_specs=[smem] + [vmem] * 2,
        out_specs=(vmem,) * 3,
        compiler_params=params,
        name="attention_own",
    )(doc_bounds, packed, own)
    attended = pl.pallas_call(
        functools.partial(attention_kernel, 1),
        out_shape=jax.ShapeDtypeStruct((Z, BLOCK, HEAD_COLS), jnp.bfloat16),
        in_specs=[smem] + [vmem] * 5,
        out_specs=vmem,
        scratch_shapes=[pltpu.VMEM((WIDE, ROWS), jnp.float32), pltpu.VMEM((1, ROWS), jnp.float32)],
        compiler_params=params,
        name="attention_other",
    )(doc_bounds, rows, top, acc, own, other)
    attended = lax.all_to_all(attended, AXES, 0, 0, axis_index_groups=groups, tiled=True)
    return attended.transpose(1, 0, 2).reshape(BLOCK, QUERY_HEADS * HEAD_SIZE)


def solution(mesh):
    split = Mesh(mesh.devices.reshape(X, Z, CORES, Y), AXES)
    rows = P(AXES, None)
    return jax.shard_map(
        on_device,
        mesh=split,
        in_specs=(rows, rows, rows, P()),
        out_specs=rows,
        check_vma=False,
    )
```

```python
import functools
import math

import jax
import jax.numpy as jnp
from jax import lax
from jax.experimental import pallas as pl
from jax.experimental.pallas import tpu as pltpu
from jax.sharding import Mesh, PartitionSpec as P

QUERY_HEADS = 32
KEY_VALUE_HEADS = 8
HEAD_SIZE = 64
DOCS = 16
GROUP = QUERY_HEADS // KEY_VALUE_HEADS

X, Z, CORES, Y = 4, 8, 2, 4
AXES = ("x", "z", "core", "y")
BLOCK = 64
TILE = Y * BLOCK
SPAN = CORES * TILE
PAIR = 2
PAIRS = Z // PAIR
PLANE = Z * SPAN
STRIDE = PAIR * SPAN
HALF = GROUP * BLOCK
ROWS = PAIR * HALF
KEYS = PAIR * TILE
WIDE = 2 * HEAD_SIZE
HEAD_COLS = GROUP * HEAD_SIZE
BASE = (3, 1, 0, 2)
BLOCKS = X * PAIRS
NEVER = 1 << 20

EXP2_SCALE = math.log2(math.e) / math.sqrt(HEAD_SIZE)
START_MAX = -1e30
HIDDEN = -3e38
LARGEST_SUM = 2.0 ** 60


def square_groups():
    groups = []
    for k in range(X):
        for core in range(CORES):
            for y in range(Y):
                groups.append([(((BASE[z // PAIR] ^ k) * Z + z) * CORES + core) * Y + y for z in range(Z)])
    return groups


def base_of(pair):
    base = jnp.int32(BASE[-1])
    for p in range(PAIRS - 1):
        base = jnp.where(pair == p, BASE[p], base)
    return base


def line_groups(first):
    index = lambda x, z, core, y: ((x * Z + z) * CORES + core) * Y + y
    groups = []
    for z in range(Z):
        for core in range(CORES):
            if (core == 0) == first:
                groups += [[index(x, z, core, y) for x in range(X)] for y in range(Y)]
            else:
                groups += [[index(x, z, core, y) for y in range(Y)] for x in range(X)]
    return groups


def doc_start(bounds, position):
    start = jnp.zeros_like(position)
    for d in range(1, DOCS):
        start = jnp.where(bounds[d] <= position, bounds[d], start)
    return start


def mix(values, weights):
    return jnp.dot(values, weights.astype(jnp.bfloat16), preferred_element_type=jnp.float32)


def attention_kernel(stage, bounds, *refs):
    if stage == 0:
        q_ref, own_ref, rows_ref, top_ref, acc_out = refs
    else:
        rows_ref, top_ref, acc_in, own_ref, other_ref, out_ref, acc_ref, run_ref = refs
    x, z, core, y = (lax.axis_index(a) for a in AXES)
    mine = base_of(lax.div(z, PAIR))
    group = x ^ mine
    column = lax.broadcasted_iota(jnp.int32, (1, WIDE), 1)
    key_lanes = (column < HEAD_SIZE).astype(jnp.bfloat16)
    value_lanes = (column >= HEAD_SIZE).astype(jnp.bfloat16)
    row = lax.broadcasted_iota(jnp.int32, (1, ROWS), 1)
    row_offset = lax.div(row, HALF) * SPAN + lax.rem(row, BLOCK)
    key = lax.broadcasted_iota(jnp.int32, (KEYS, WIDE), 0)
    key_offset = lax.div(key, TILE) * SPAN + lax.rem(key, TILE)
    kv_ref, offset = (own_ref, core) if stage == 0 else (other_ref, 1 - core)

    def one_pair(p, _):
        plane = base_of(p) ^ group
        home = plane * PAIRS + p
        first = home * STRIDE + core * TILE + y * BLOCK
        start = doc_start(bounds, first)
        begin = lax.div(start, STRIDE)
        one_document = start == doc_start(bounds, first + SPAN + BLOCK - 1)

        after = jnp.where(column == HEAD_SIZE + 1, first, jnp.where(column == HEAD_SIZE + 2, first + SPAN, NEVER))
        held = jnp.where(column == HEAD_SIZE, first, NEVER)

        def load(kv_ref, offset, blocks, limits=None):
            parts, masks, origins = [], [], []
            for n, block in enumerate(blocks):
                near = jnp.minimum(block, BLOCKS - 1)
                q = lax.rem(near, PAIRS)
                source = lax.div(near, PAIRS) ^ base_of(q) ^ mine
                for g in range(PAIR):
                    for i in range(Y):
                        at = jnp.where(offset == 0, i * X + source, source * Y + i)
                        parts.append(kv_ref[at, q * PAIR + g])
                origin = block * STRIDE + offset * TILE
                origins.append(origin)
                if limits is not None:
                    before = jnp.where(column == HEAD_SIZE, limits[n] - origin, -NEVER)
                    unseen = (key_offset < before) | (key_offset >= after - origin)
                    if stage == 0:
                        unseen = unseen | ((key_offset >= held - origin) & (key_offset < held + BLOCK - origin))
                    masks.append(jnp.where(unseen, START_MAX, 0.0))
            kv = jnp.concatenate(parts, axis=0)
            keys = kv * key_lanes
            if limits is not None:
                keys = keys + jnp.concatenate(masks, axis=0).astype(jnp.bfloat16)
            return keys, (kv * value_lanes + key_lanes).T, origins

        def across(origins, low, high=None):
            offsets = jnp.concatenate([key_offset] * (ROWS // WIDE), axis=1)
            seen = []
            for origin in origins:
                inside = offsets >= low - origin
                seen.append(inside if high is None else inside & (offsets <= high - origin))
            return seen

        def hide(scores, seen):
            parts = [jnp.where(m, scores[n * KEYS:(n + 1) * KEYS], HIDDEN) for n, m in enumerate(seen)]
            return jnp.concatenate(parts, axis=0)

        if stage == 0:
            line = lax.broadcasted_iota(jnp.int32, (HEAD_SIZE, ROWS), 0)
            half = lax.broadcasted_iota(jnp.int32, (HEAD_SIZE, ROWS), 1) // HALF
            filler = ((line == 0) | (line == half + 1)).astype(jnp.bfloat16)
            own = [q_ref[PAIR * p + b] for b in range(PAIR)]
            pieces = []
            for block in own:
                turned = block[:, WIDE:].T
                pieces += [turned[j * HEAD_SIZE:(j + 1) * HEAD_SIZE] for j in range(GROUP)]
            rows = jnp.concatenate([jnp.concatenate(pieces, axis=1), filler], axis=0)
            rows_ref[p] = rows
            kv = jnp.concatenate([block[:, :WIDE] for block in own], axis=0)
            k = lax.broadcasted_iota(jnp.int32, (PAIR * BLOCK, 1), 0)
            k_offset = lax.div(k, BLOCK) * SPAN + lax.rem(k, BLOCK)
            scores = jnp.dot(kv * key_lanes, rows, preferred_element_type=jnp.float32)
            lo = doc_start(bounds, first + row_offset) - first
            scores = jnp.where((k_offset >= lo) & (k_offset <= row_offset), scores, HIDDEN)
            top = jnp.max(scores, axis=0, keepdims=True)
            top_ref[p] = top
            acc = acc_out.at[p]
            acc[...] = mix((kv * value_lanes + key_lanes).T, jnp.exp2(scores * EXP2_SCALE - top * EXP2_SCALE))
        else:
            acc = acc_ref
            acc[...] = acc_in[p]

        def add(blocks, limits=None, lo=None):
            keys, values, origins = load(kv_ref, offset, blocks, limits)
            scores = jnp.dot(keys, rows_ref[p], preferred_element_type=jnp.float32)
            if lo is not None:
                scores = hide(scores, across(origins, lo))
            weights = jnp.exp2(scores * EXP2_SCALE - top_ref[p] * EXP2_SCALE)
            acc[...] += mix(values, weights)

        @pl.when(one_document)
        def _():
            add([home, begin], [start, jnp.where(begin == home, NEVER, start)])
            inside = home - begin - 1

            def step(s, _):
                add([begin + 1 + 2 * s, begin + 2 + 2 * s])
                return 0

            lax.fori_loop(0, lax.div(inside, 2), step, 0)

            @pl.when((inside > 0) & (lax.rem(inside, 2) == 1))
            def _():
                add([home - 1])

        @pl.when(jnp.logical_not(one_document))
        def _():
            lo = doc_start(bounds, first + row_offset)

            count = home - begin + 1

            def step(s, _):
                add([begin + 2 * s, begin + 2 * s + 1], [start, start], lo)
                return 0

            lax.fori_loop(0, lax.div(count, 2), step, 0)

            @pl.when(lax.rem(count, 2) == 1)
            def _():
                add([home], [start], lo)

        if stage == 0:
            return 0

        within = jnp.min((acc[0:1, :] <= LARGEST_SUM).astype(jnp.float32))

        @pl.when(within < 0.5)
        def _():
            hi = first + row_offset
            lo = doc_start(bounds, hi)
            acc[...] = jnp.zeros_like(acc)
            run_ref[...] = jnp.full(run_ref.shape, START_MAX, jnp.float32)
            for again_ref, again_offset in ((own_ref, core), (other_ref, 1 - core)):
                def step(block, _):
                    keys, values, origins = load(again_ref, again_offset, [block])
                    scores = jnp.dot(keys, rows_ref[p], preferred_element_type=jnp.float32)
                    scores = hide(scores, across(origins, lo, hi))
                    top = run_ref[...]
                    new_top = jnp.maximum(top, jnp.max(scores, axis=0, keepdims=True))
                    shrink = jnp.exp2((top - new_top) * EXP2_SCALE)
                    acc[...] = acc[...] * shrink + mix(values, jnp.exp2((scores - new_top) * EXP2_SCALE))
                    run_ref[...] = new_top
                    return 0

                lax.fori_loop(begin, home + 1, step, 0)

        result = (acc[HEAD_SIZE:, :] / acc[0:1, :]).T
        for b in range(PAIR):
            heads = [result[(b * GROUP + j) * BLOCK:(b * GROUP + j + 1) * BLOCK] for j in range(GROUP)]
            out_ref[PAIR * p + b] = jnp.concatenate(heads, axis=1).astype(jnp.bfloat16)
        return 0

    lax.fori_loop(0, PAIRS, one_pair, 0)


def pack_kernel(q_ref, k_ref, v_ref, out_ref):
    for h in range(KEY_VALUE_HEADS):
        cols = slice(h * HEAD_SIZE, (h + 1) * HEAD_SIZE)
        out_ref[h, :, :WIDE] = jnp.concatenate([k_ref[:, cols], v_ref[:, cols]], axis=1)
        out_ref[h, :, WIDE:] = q_ref[:, h * HEAD_COLS:(h + 1) * HEAD_COLS]


def on_device(queries, keys, values, doc_bounds):
    smem = pl.BlockSpec(memory_space=pltpu.SMEM)
    vmem = pl.BlockSpec(memory_space=pltpu.VMEM)
    groups = square_groups()
    packed = pl.pallas_call(
        pack_kernel,
        out_shape=pltpu.VMEM((Z, BLOCK, WIDE + HEAD_COLS), jnp.bfloat16),
        in_specs=[vmem] * 3,
        out_specs=vmem,
        name="pack",
    )(queries, keys, values)
    packed = lax.all_to_all(packed, AXES, 0, 0, axis_index_groups=groups, tiled=True)
    gathered = packed[:, :, :WIDE]
    for first in (True, False):
        copies = jnp.broadcast_to(gathered[None], (X,) + gathered.shape)
        gathered = lax.all_to_all(copies, AXES, 0, 0, axis_index_groups=line_groups(first), tiled=True)
    own = gathered.reshape(X * Y, Z, BLOCK, WIDE)
    other = lax.ppermute(own, "core", [(0, 1), (1, 0)])

    acc_shape = jax.ShapeDtypeStruct((PAIRS, WIDE, ROWS), jnp.float32)
    top_shape = jax.ShapeDtypeStruct((PAIRS, 1, ROWS), jnp.float32)
    rows_shape = jax.ShapeDtypeStruct((PAIRS, WIDE, ROWS), jnp.bfloat16)
    params = pltpu.CompilerParams(vmem_limit_bytes=40 * 1024 * 1024)
    rows, top, acc = pl.pallas_call(
        functools.partial(attention_kernel, 0),
        out_shape=(rows_shape, top_shape, acc_shape),
        in_specs=[smem] + [vmem] * 2,
        out_specs=(vmem,) * 3,
        compiler_params=params,
        name="attention_own",
    )(doc_bounds, packed, own)
    attended = pl.pallas_call(
        functools.partial(attention_kernel, 1),
        out_shape=jax.ShapeDtypeStruct((Z, BLOCK, HEAD_COLS), jnp.bfloat16),
        in_specs=[smem] + [vmem] * 5,
        out_specs=vmem,
        scratch_shapes=[pltpu.VMEM((WIDE, ROWS), jnp.float32), pltpu.VMEM((1, ROWS), jnp.float32)],
        compiler_params=params,
        name="attention_other",
    )(doc_bounds, rows, top, acc, own, other)
    attended = lax.all_to_all(attended, AXES, 0, 0, axis_index_groups=groups, tiled=True)
    return attended.transpose(1, 0, 2).reshape(BLOCK, QUERY_HEADS * HEAD_SIZE)


def solution(mesh):
    split = Mesh(mesh.devices.reshape(X, Z, CORES, Y), AXES)
    rows = P(AXES, None)
    return jax.shard_map(
        on_device,
        mesh=split,
        in_specs=(rows, rows, rows, P()),
        out_specs=rows,
        check_vma=False,
    )
```

```python
import functools
import math

import jax
import jax.numpy as jnp
from jax import lax
from jax.experimental import pallas as pl
from jax.experimental.pallas import tpu as pltpu
from jax.sharding import Mesh, PartitionSpec as P

QUERY_HEADS = 32
KEY_VALUE_HEADS = 8
HEAD_SIZE = 64
DOCS = 16
GROUP = QUERY_HEADS // KEY_VALUE_HEADS

X, Z, CORES, Y = 4, 8, 2, 4
AXES = ("x", "z", "core", "y")
BLOCK = 64
TILE = Y * BLOCK
SPAN = CORES * TILE
PAIR = 2
PAIRS = Z // PAIR
PLANE = Z * SPAN
STRIDE = PAIR * SPAN
HALF = GROUP * BLOCK
ROWS = PAIR * HALF
KEYS = PAIR * TILE
WIDE = 2 * HEAD_SIZE
HEAD_COLS = GROUP * HEAD_SIZE
BASE = (3, 1, 0, 2)
BLOCKS = X * PAIRS
NEVER = 1 << 20

EXP2_SCALE = math.log2(math.e) / math.sqrt(HEAD_SIZE)
START_MAX = -1e30
HIDDEN = -3e38
LARGEST_SUM = 2.0 ** 60


def square_groups():
    groups = []
    for k in range(X):
        for core in range(CORES):
            for y in range(Y):
                groups.append([(((BASE[z // PAIR] ^ k) * Z + z) * CORES + core) * Y + y for z in range(Z)])
    return groups


def base_of(pair):
    base = jnp.int32(BASE[-1])
    for p in range(PAIRS - 1):
        base = jnp.where(pair == p, BASE[p], base)
    return base


def line_groups(first):
    index = lambda x, z, core, y: ((x * Z + z) * CORES + core) * Y + y
    groups = []
    for z in range(Z):
        for core in range(CORES):
            if (core == 0) == first:
                groups += [[index(x, z, core, y) for x in range(X)] for y in range(Y)]
            else:
                groups += [[index(x, z, core, y) for y in range(Y)] for x in range(X)]
    return groups


def doc_start(bounds, position):
    start = jnp.zeros_like(position)
    for d in range(1, DOCS):
        start = jnp.where(bounds[d] <= position, bounds[d], start)
    return start


def mix(values, weights):
    return jnp.dot(values, weights.astype(jnp.bfloat16), preferred_element_type=jnp.float32)


def attention_kernel(stage, bounds, *refs):
    if stage == 0:
        q_ref, own_ref, rows_ref, top_ref, acc_out = refs
    else:
        rows_ref, top_ref, acc_in, own_ref, other_ref, out_ref, acc_ref, run_ref = refs
    x, z, core, y = (lax.axis_index(a) for a in AXES)
    mine = base_of(lax.div(z, PAIR))
    group = x ^ mine
    column = lax.broadcasted_iota(jnp.int32, (1, WIDE), 1)
    key_lanes = (column < HEAD_SIZE).astype(jnp.bfloat16)
    value_lanes = (column >= HEAD_SIZE).astype(jnp.bfloat16)
    row = lax.broadcasted_iota(jnp.int32, (1, ROWS), 1)
    row_offset = lax.div(row, HALF) * SPAN + lax.rem(row, BLOCK)
    key = lax.broadcasted_iota(jnp.int32, (KEYS, WIDE), 0)
    key_offset = lax.div(key, TILE) * SPAN + lax.rem(key, TILE)
    kv_ref, offset = (own_ref, core) if stage == 0 else (other_ref, 1 - core)

    def one_pair(p, _):
        plane = base_of(p) ^ group
        home = plane * PAIRS + p
        first = home * STRIDE + core * TILE + y * BLOCK
        start = doc_start(bounds, first)
        begin = lax.div(start, STRIDE)
        one_document = start == doc_start(bounds, first + SPAN + BLOCK - 1)

        after = jnp.where(column == HEAD_SIZE + 1, first, jnp.where(column == HEAD_SIZE + 2, first + SPAN, NEVER))
        held = jnp.where(column == HEAD_SIZE, first, NEVER)

        def load(kv_ref, offset, blocks, limits=None):
            parts, masks, origins = [], [], []
            for n, block in enumerate(blocks):
                near = jnp.minimum(block, BLOCKS - 1)
                q = lax.rem(near, PAIRS)
                source = lax.div(near, PAIRS) ^ base_of(q) ^ mine
                for g in range(PAIR):
                    for i in range(Y):
                        at = jnp.where(offset == 0, i * X + source, source * Y + i)
                        parts.append(kv_ref[at, q * PAIR + g])
                origin = block * STRIDE + offset * TILE
                origins.append(origin)
                if limits is not None:
                    before = jnp.where(column == HEAD_SIZE, limits[n] - origin, -NEVER)
                    unseen = (key_offset < before) | (key_offset >= after - origin)
                    if stage == 0:
                        unseen = unseen | ((key_offset >= held - origin) & (key_offset < held + BLOCK - origin))
                    masks.append(jnp.where(unseen, START_MAX, 0.0))
            kv = jnp.concatenate(parts, axis=0)
            keys = kv * key_lanes
            if limits is not None:
                keys = keys + jnp.concatenate(masks, axis=0).astype(jnp.bfloat16)
            return keys, (kv * value_lanes + key_lanes).T, origins

        def across(origins, low, high=None):
            offsets = jnp.concatenate([key_offset] * (ROWS // WIDE), axis=1)
            seen = []
            for origin in origins:
                inside = offsets >= low - origin
                seen.append(inside if high is None else inside & (offsets <= high - origin))
            return seen

        def hide(scores, seen):
            parts = [jnp.where(m, scores[n * KEYS:(n + 1) * KEYS], HIDDEN) for n, m in enumerate(seen)]
            return jnp.concatenate(parts, axis=0)

        if stage == 0:
            line = lax.broadcasted_iota(jnp.int32, (HEAD_SIZE, ROWS), 0)
            half = lax.broadcasted_iota(jnp.int32, (HEAD_SIZE, ROWS), 1) // HALF
            filler = ((line == 0) | (line == half + 1)).astype(jnp.bfloat16)
            own = [q_ref[PAIR * p + b] for b in range(PAIR)]
            pieces = []
            for block in own:
                turned = block[:, WIDE:].T
                pieces += [turned[j * HEAD_SIZE:(j + 1) * HEAD_SIZE] for j in range(GROUP)]
            rows = jnp.concatenate([jnp.concatenate(pieces, axis=1), filler], axis=0)
            rows_ref[p] = rows
            kv = jnp.concatenate([block[:, :WIDE] for block in own], axis=0)
            k = lax.broadcasted_iota(jnp.int32, (PAIR * BLOCK, 1), 0)
            k_offset = lax.div(k, BLOCK) * SPAN + lax.rem(k, BLOCK)
            scores = jnp.dot(kv * key_lanes, rows, preferred_element_type=jnp.float32)
            lo = doc_start(bounds, first + row_offset) - first
            scores = jnp.where((k_offset >= lo) & (k_offset <= row_offset), scores, HIDDEN)
            top = jnp.max(scores, axis=0, keepdims=True)
            top_ref[p] = top
            acc = acc_out.at[p]
            acc[...] = mix((kv * value_lanes + key_lanes).T, jnp.exp2(scores * EXP2_SCALE - top * EXP2_SCALE))
        else:
            acc = acc_ref
            acc[...] = acc_in[p]

        def add(blocks, limits=None, lo=None):
            keys, values, origins = load(kv_ref, offset, blocks, limits)
            scores = jnp.dot(keys, rows_ref[p], preferred_element_type=jnp.float32)
            if lo is not None:
                scores = hide(scores, across(origins, lo))
            weights = jnp.exp2(scores * EXP2_SCALE - top_ref[p] * EXP2_SCALE)
            acc[...] += mix(values, weights)

        @pl.when(one_document)
        def _():
            add([home, begin], [start, jnp.where(begin == home, NEVER, start)])
            inside = home - begin - 1

            def step(s, _):
                add([begin + 1 + 4 * s + n for n in range(4)])
                return 0

            lax.fori_loop(0, lax.div(inside, 4), step, 0)

            @pl.when((inside > 0) & (lax.rem(inside, 4) >= 2))
            def _():
                left = begin + 1 + inside - lax.rem(inside, 4)
                add([left, left + 1])

            @pl.when((inside > 0) & (lax.rem(inside, 2) == 1))
            def _():
                add([home - 1])

        @pl.when(jnp.logical_not(one_document))
        def _():
            lo = doc_start(bounds, first + row_offset)

            count = home - begin + 1

            def step(s, _):
                add([begin + 2 * s, begin + 2 * s + 1], [start, start], lo)
                return 0

            lax.fori_loop(0, lax.div(count, 2), step, 0)

            @pl.when(lax.rem(count, 2) == 1)
            def _():
                add([home], [start], lo)

        if stage == 0:
            return 0

        within = jnp.min((acc[0:1, :] <= LARGEST_SUM).astype(jnp.float32))

        @pl.when(within < 0.5)
        def _():
            hi = first + row_offset
            lo = doc_start(bounds, hi)
            acc[...] = jnp.zeros_like(acc)
            run_ref[...] = jnp.full(run_ref.shape, START_MAX, jnp.float32)
            for again_ref, again_offset in ((own_ref, core), (other_ref, 1 - core)):
                def step(block, _):
                    keys, values, origins = load(again_ref, again_offset, [block])
                    scores = jnp.dot(keys, rows_ref[p], preferred_element_type=jnp.float32)
                    scores = hide(scores, across(origins, lo, hi))
                    top = run_ref[...]
                    new_top = jnp.maximum(top, jnp.max(scores, axis=0, keepdims=True))
                    shrink = jnp.exp2((top - new_top) * EXP2_SCALE)
                    acc[...] = acc[...] * shrink + mix(values, jnp.exp2((scores - new_top) * EXP2_SCALE))
                    run_ref[...] = new_top
                    return 0

                lax.fori_loop(begin, home + 1, step, 0)

        result = (acc[HEAD_SIZE:, :] / acc[0:1, :]).T
        for b in range(PAIR):
            heads = [result[(b * GROUP + j) * BLOCK:(b * GROUP + j + 1) * BLOCK] for j in range(GROUP)]
            out_ref[PAIR * p + b] = jnp.concatenate(heads, axis=1).astype(jnp.bfloat16)
        return 0

    lax.fori_loop(0, PAIRS, one_pair, 0)


def pack_kernel(q_ref, k_ref, v_ref, out_ref):
    for h in range(KEY_VALUE_HEADS):
        cols = slice(h * HEAD_SIZE, (h + 1) * HEAD_SIZE)
        out_ref[h, :, :WIDE] = jnp.concatenate([k_ref[:, cols], v_ref[:, cols]], axis=1)
        out_ref[h, :, WIDE:] = q_ref[:, h * HEAD_COLS:(h + 1) * HEAD_COLS]


def on_device(queries, keys, values, doc_bounds):
    smem = pl.BlockSpec(memory_space=pltpu.SMEM)
    vmem = pl.BlockSpec(memory_space=pltpu.VMEM)
    groups = square_groups()
    packed = pl.pallas_call(
        pack_kernel,
        out_shape=pltpu.VMEM((Z, BLOCK, WIDE + HEAD_COLS), jnp.bfloat16),
        in_specs=[vmem] * 3,
        out_specs=vmem,
        name="pack",
    )(queries, keys, values)
    packed = lax.all_to_all(packed, AXES, 0, 0, axis_index_groups=groups, tiled=True)
    gathered = packed[:, :, :WIDE]
    for first in (True, False):
        copies = jnp.broadcast_to(gathered[None], (X,) + gathered.shape)
        gathered = lax.all_to_all(copies, AXES, 0, 0, axis_index_groups=line_groups(first), tiled=True)
    own = gathered.reshape(X * Y, Z, BLOCK, WIDE)
    other = lax.ppermute(own, "core", [(0, 1), (1, 0)])

    acc_shape = jax.ShapeDtypeStruct((PAIRS, WIDE, ROWS), jnp.float32)
    top_shape = jax.ShapeDtypeStruct((PAIRS, 1, ROWS), jnp.float32)
    rows_shape = jax.ShapeDtypeStruct((PAIRS, WIDE, ROWS), jnp.bfloat16)
    params = pltpu.CompilerParams(
        vmem_limit_bytes=40 * 1024 * 1024,
    )
    rows, top, acc = pl.pallas_call(
        functools.partial(attention_kernel, 0),
        out_shape=(rows_shape, top_shape, acc_shape),
        in_specs=[smem] + [vmem] * 2,
        out_specs=(vmem,) * 3,
        compiler_params=params,
        name="attention_own",
    )(doc_bounds, packed, own)
    attended = pl.pallas_call(
        functools.partial(attention_kernel, 1),
        out_shape=jax.ShapeDtypeStruct((Z, BLOCK, HEAD_COLS), jnp.bfloat16),
        in_specs=[smem] + [vmem] * 5,
        out_specs=vmem,
        scratch_shapes=[pltpu.VMEM((WIDE, ROWS), jnp.float32), pltpu.VMEM((1, ROWS), jnp.float32)],
        compiler_params=params,
        name="attention_other",
    )(doc_bounds, rows, top, acc, own, other)
    attended = lax.all_to_all(attended, AXES, 0, 0, axis_index_groups=groups, tiled=True)
    return attended.transpose(1, 0, 2).reshape(BLOCK, QUERY_HEADS * HEAD_SIZE)


def solution(mesh):
    split = Mesh(mesh.devices.reshape(X, Z, CORES, Y), AXES)
    rows = P(AXES, None)
    return jax.shard_map(
        on_device,
        mesh=split,
        in_specs=(rows, rows, rows, P()),
        out_specs=rows,
        check_vma=False,
    )
```

```python
import functools
import math

import jax
import jax.numpy as jnp
from jax import lax
from jax.experimental import pallas as pl
from jax.experimental.pallas import tpu as pltpu
from jax.sharding import Mesh, PartitionSpec as P


QUERY_HEADS = 32
KEY_VALUE_HEADS = 8
HEAD_SIZE = 64
DOCS = 16
GROUP = QUERY_HEADS // KEY_VALUE_HEADS

X, Z, CORES, Y = 4, 8, 2, 4
AXES = ("x", "z", "core", "y")
BLOCK = 64
TILE = Y * BLOCK
SPAN = CORES * TILE
PAIR = 2
PAIRS = Z // PAIR
PLANE = Z * SPAN
STRIDE = PAIR * SPAN
HALF = GROUP * BLOCK
ROWS = PAIR * HALF
KEYS = PAIR * TILE
WIDE = 2 * HEAD_SIZE
HEAD_COLS = GROUP * HEAD_SIZE
BASE = (3, 1, 0, 2)
BLOCKS = X * PAIRS
NEVER = 1 << 20

EXP2_SCALE = math.log2(math.e) / math.sqrt(HEAD_SIZE)
START_MAX = -1e30
HIDDEN = -3e38
LARGEST_SUM = 2.0 ** 60


def square_groups():
    groups = []
    for k in range(X):
        for core in range(CORES):
            for y in range(Y):
                groups.append([(((BASE[z // PAIR] ^ k) * Z + z) * CORES + core) * Y + y for z in range(Z)])
    return groups


def base_of(pair):
    base = jnp.int32(BASE[-1])
    for p in range(PAIRS - 1):
        base = jnp.where(pair == p, BASE[p], base)
    return base


def line_groups(first):
    index = lambda x, z, core, y: ((x * Z + z) * CORES + core) * Y + y
    groups = []
    for z in range(Z):
        for core in range(CORES):
            if (core == 0) == first:
                groups += [[index(x, z, core, y) for x in range(X)] for y in range(Y)]
            else:
                groups += [[index(x, z, core, y) for y in range(Y)] for x in range(X)]
    return groups


def doc_start(bounds, position):
    start = jnp.zeros_like(position)
    for d in range(1, DOCS):
        start = jnp.where(bounds[d] <= position, bounds[d], start)
    return start


def mix(values, weights):
    return jnp.dot(values, weights.astype(jnp.bfloat16), preferred_element_type=jnp.float32)


def start_kernel(bounds, q_ref, rows_ref, top_ref, acc_ref):
    x, z, core, y = (lax.axis_index(a) for a in AXES)
    group = x ^ base_of(lax.div(z, PAIR))
    column = lax.broadcasted_iota(jnp.int32, (1, WIDE), 1)
    key_lanes = (column < HEAD_SIZE).astype(jnp.bfloat16)
    value_lanes = (column >= HEAD_SIZE).astype(jnp.bfloat16)
    row = lax.broadcasted_iota(jnp.int32, (1, ROWS), 1)
    row_offset = lax.div(row, HALF) * SPAN + lax.rem(row, BLOCK)

    def one_pair(p, _):
        first = (base_of(p) ^ group) * PLANE + p * STRIDE + core * TILE + y * BLOCK
        line = lax.broadcasted_iota(jnp.int32, (HEAD_SIZE, ROWS), 0)
        half = lax.broadcasted_iota(jnp.int32, (HEAD_SIZE, ROWS), 1) // HALF
        filler = ((line == 0) | (line == half + 1)).astype(jnp.bfloat16)
        own = [q_ref[PAIR * p + b] for b in range(PAIR)]
        pieces = []
        for block in own:
            turned = block[:, WIDE:].T
            pieces += [turned[j * HEAD_SIZE:(j + 1) * HEAD_SIZE] for j in range(GROUP)]
        rows = jnp.concatenate([jnp.concatenate(pieces, axis=1), filler], axis=0)
        rows_ref[p] = rows
        kv = jnp.concatenate([block[:, :WIDE] for block in own], axis=0)
        k = lax.broadcasted_iota(jnp.int32, (PAIR * BLOCK, 1), 0)
        k_offset = lax.div(k, BLOCK) * SPAN + lax.rem(k, BLOCK)
        scores = jnp.dot(kv * key_lanes, rows, preferred_element_type=jnp.float32)
        lo = doc_start(bounds, first + row_offset) - first
        scores = jnp.where((k_offset >= lo) & (k_offset <= row_offset), scores, HIDDEN)
        top = jnp.max(scores, axis=0, keepdims=True)
        top_ref[p] = top
        acc_ref[p] = mix((kv * value_lanes + key_lanes).T, jnp.exp2(scores * EXP2_SCALE - top * EXP2_SCALE))
        return 0

    lax.fori_loop(0, PAIRS, one_pair, 0)


def attention_kernel(stage, bounds, *refs):
    if stage == 0:
        rows_ref, top_ref, acc_in, own_ref, acc_out = refs
    else:
        rows_ref, top_ref, acc_in, own_ref, other_ref, out_ref, acc_ref, run_ref = refs
    x, z, core, y = (lax.axis_index(a) for a in AXES)
    mine = base_of(lax.div(z, PAIR))
    group = x ^ mine
    column = lax.broadcasted_iota(jnp.int32, (1, WIDE), 1)
    key_lanes = (column < HEAD_SIZE).astype(jnp.bfloat16)
    value_lanes = (column >= HEAD_SIZE).astype(jnp.bfloat16)
    row = lax.broadcasted_iota(jnp.int32, (1, ROWS), 1)
    row_offset = lax.div(row, HALF) * SPAN + lax.rem(row, BLOCK)
    key = lax.broadcasted_iota(jnp.int32, (KEYS, WIDE), 0)
    key_offset = lax.div(key, TILE) * SPAN + lax.rem(key, TILE)
    kv_ref, offset = (own_ref, core) if stage == 0 else (other_ref, 1 - core)

    def one_pair(p, _):
        plane = base_of(p) ^ group
        home = plane * PAIRS + p
        first = home * STRIDE + core * TILE + y * BLOCK
        start = doc_start(bounds, first)
        begin = lax.div(start, STRIDE)
        one_document = start == doc_start(bounds, first + SPAN + BLOCK - 1)

        after = jnp.where(column == HEAD_SIZE + 1, first, jnp.where(column == HEAD_SIZE + 2, first + SPAN, NEVER))
        held = jnp.where(column == HEAD_SIZE, first, NEVER)

        def load(kv_ref, offset, blocks, limits=None):
            parts, masks, origins = [], [], []
            for n, block in enumerate(blocks):
                near = jnp.minimum(block, BLOCKS - 1)
                q = lax.rem(near, PAIRS)
                source = lax.div(near, PAIRS) ^ base_of(q) ^ mine
                for g in range(PAIR):
                    for i in range(Y):
                        at = jnp.where(offset == 0, i * X + source, source * Y + i)
                        parts.append(kv_ref[at, q * PAIR + g])
                origin = block * STRIDE + offset * TILE
                origins.append(origin)
                if limits is not None:
                    before = jnp.where(column == HEAD_SIZE, limits[n] - origin, -NEVER)
                    unseen = (key_offset < before) | (key_offset >= after - origin)
                    if stage == 0:
                        unseen = unseen | ((key_offset >= held - origin) & (key_offset < held + BLOCK - origin))
                    masks.append(jnp.where(unseen, START_MAX, 0.0))
            kv = jnp.concatenate(parts, axis=0)
            keys = kv * key_lanes
            if limits is not None:
                keys = keys + jnp.concatenate(masks, axis=0).astype(jnp.bfloat16)
            return keys, (kv * value_lanes + key_lanes).T, origins

        def across(origins, low, high=None):
            offsets = jnp.concatenate([key_offset] * (ROWS // WIDE), axis=1)
            seen = []
            for origin in origins:
                inside = offsets >= low - origin
                seen.append(inside if high is None else inside & (offsets <= high - origin))
            return seen

        def hide(scores, seen):
            parts = [jnp.where(m, scores[n * KEYS:(n + 1) * KEYS], HIDDEN) for n, m in enumerate(seen)]
            return jnp.concatenate(parts, axis=0)

        if stage == 0:
            acc = acc_out.at[p]
        else:
            acc = acc_ref
        acc[...] = acc_in[p]

        def add(blocks, limits=None, lo=None):
            keys, values, origins = load(kv_ref, offset, blocks, limits)
            scores = jnp.dot(keys, rows_ref[p], preferred_element_type=jnp.float32)
            if lo is not None:
                scores = hide(scores, across(origins, lo))
            weights = jnp.exp2(scores * EXP2_SCALE - top_ref[p] * EXP2_SCALE)
            acc[...] += mix(values, weights)

        @pl.when(one_document)
        def _():
            add([home, begin], [start, jnp.where(begin == home, NEVER, start)])
            inside = home - begin - 1

            def step(s, _):
                add([begin + 1 + 4 * s + n for n in range(4)])
                return 0

            lax.fori_loop(0, lax.div(inside, 4), step, 0)

            @pl.when((inside > 0) & (lax.rem(inside, 4) >= 2))
            def _():
                left = begin + 1 + inside - lax.rem(inside, 4)
                add([left, left + 1])

            @pl.when((inside > 0) & (lax.rem(inside, 2) == 1))
            def _():
                add([home - 1])

        @pl.when(jnp.logical_not(one_document))
        def _():
            lo = doc_start(bounds, first + row_offset)

            count = home - begin + 1

            def step(s, _):
                add([begin + 2 * s, begin + 2 * s + 1], [start, start], lo)
                return 0

            lax.fori_loop(0, lax.div(count, 2), step, 0)

            @pl.when(lax.rem(count, 2) == 1)
            def _():
                add([home], [start], lo)

        if stage == 0:
            return 0

        within = jnp.min((acc[0:1, :] <= LARGEST_SUM).astype(jnp.float32))

        @pl.when(within < 0.5)
        def _():
            hi = first + row_offset
            lo = doc_start(bounds, hi)
            acc[...] = jnp.zeros_like(acc)
            run_ref[...] = jnp.full(run_ref.shape, START_MAX, jnp.float32)
            for again_ref, again_offset in ((own_ref, core), (other_ref, 1 - core)):
                def step(block, _):
                    keys, values, origins = load(again_ref, again_offset, [block])
                    scores = jnp.dot(keys, rows_ref[p], preferred_element_type=jnp.float32)
                    scores = hide(scores, across(origins, lo, hi))
                    top = run_ref[...]
                    new_top = jnp.maximum(top, jnp.max(scores, axis=0, keepdims=True))
                    shrink = jnp.exp2((top - new_top) * EXP2_SCALE)
                    acc[...] = acc[...] * shrink + mix(values, jnp.exp2((scores - new_top) * EXP2_SCALE))
                    run_ref[...] = new_top
                    return 0

                lax.fori_loop(begin, home + 1, step, 0)

        result = (acc[HEAD_SIZE:, :] / acc[0:1, :]).T
        for b in range(PAIR):
            heads = [result[(b * GROUP + j) * BLOCK:(b * GROUP + j + 1) * BLOCK] for j in range(GROUP)]
            out_ref[PAIR * p + b] = jnp.concatenate(heads, axis=1).astype(jnp.bfloat16)
        return 0

    lax.fori_loop(0, PAIRS, one_pair, 0)


def pack_kernel(q_ref, k_ref, v_ref, out_ref):
    for h in range(KEY_VALUE_HEADS):
        cols = slice(h * HEAD_SIZE, (h + 1) * HEAD_SIZE)
        out_ref[h, :, :WIDE] = jnp.concatenate([k_ref[:, cols], v_ref[:, cols]], axis=1)
        out_ref[h, :, WIDE:] = q_ref[:, h * HEAD_COLS:(h + 1) * HEAD_COLS]


def on_device(queries, keys, values, doc_bounds):
    smem = pl.BlockSpec(memory_space=pltpu.SMEM)
    vmem = pl.BlockSpec(memory_space=pltpu.VMEM)
    groups = square_groups()
    packed = pl.pallas_call(
        pack_kernel,
        out_shape=pltpu.VMEM((Z, BLOCK, WIDE + HEAD_COLS), jnp.bfloat16),
        in_specs=[vmem] * 3,
        out_specs=vmem,
        name="pack",
    )(queries, keys, values)
    packed = lax.all_to_all(packed, AXES, 0, 0, axis_index_groups=groups, tiled=True)
    gathered = packed[:, :, :WIDE]
    for first in (True, False):
        copies = jnp.broadcast_to(gathered[None], (X,) + gathered.shape)
        gathered = lax.all_to_all(copies, AXES, 0, 0, axis_index_groups=line_groups(first), tiled=True)
    own = gathered.reshape(X * Y, Z, BLOCK, WIDE)
    other = lax.ppermute(own, "core", [(0, 1), (1, 0)])

    acc_shape = jax.ShapeDtypeStruct((PAIRS, WIDE, ROWS), jnp.float32)
    top_shape = jax.ShapeDtypeStruct((PAIRS, 1, ROWS), jnp.float32)
    rows_shape = jax.ShapeDtypeStruct((PAIRS, WIDE, ROWS), jnp.bfloat16)
    params = pltpu.CompilerParams(vmem_limit_bytes=40 * 1024 * 1024)
    rows, top, acc = pl.pallas_call(
        start_kernel,
        out_shape=tuple(pltpu.VMEM(a.shape, a.dtype) for a in (rows_shape, top_shape, acc_shape)),
        in_specs=[smem, vmem],
        out_specs=(vmem,) * 3,
        name="attention_start",
    )(doc_bounds, packed)
    acc = pl.pallas_call(
        functools.partial(attention_kernel, 0),
        out_shape=acc_shape,
        in_specs=[smem] + [vmem] * 4,
        out_specs=vmem,
        compiler_params=params,
        name="attention_own",
    )(doc_bounds, rows, top, acc, own)
    attended = pl.pallas_call(
        functools.partial(attention_kernel, 1),
        out_shape=jax.ShapeDtypeStruct((Z, BLOCK, HEAD_COLS), jnp.bfloat16),
        in_specs=[smem] + [vmem] * 5,
        out_specs=vmem,
        scratch_shapes=[pltpu.VMEM((WIDE, ROWS), jnp.float32), pltpu.VMEM((1, ROWS), jnp.float32)],
        compiler_params=params,
        name="attention_other",
    )(doc_bounds, rows, top, acc, own, other)
    attended = lax.all_to_all(attended, AXES, 0, 0, axis_index_groups=groups, tiled=True)
    return attended.transpose(1, 0, 2).reshape(BLOCK, QUERY_HEADS * HEAD_SIZE)


def solution(mesh):
    split = Mesh(mesh.devices.reshape(X, Z, CORES, Y), AXES)
    rows = P(AXES, None)
    return jax.shard_map(
        on_device,
        mesh=split,
        in_specs=(rows, rows, rows, P()),
        out_specs=rows,
        check_vma=False,
    )
```

```python
import functools
import math

import jax
import jax.numpy as jnp
from jax import lax
from jax.experimental import pallas as pl
from jax.experimental.pallas import tpu as pltpu
from jax.sharding import Mesh, PartitionSpec as P


QUERY_HEADS = 32
KEY_VALUE_HEADS = 8
HEAD_SIZE = 64
DOCS = 16
GROUP = QUERY_HEADS // KEY_VALUE_HEADS

X, Z, CORES, Y = 4, 8, 2, 4
AXES = ("x", "z", "core", "y")
BLOCK = 64
TILE = Y * BLOCK
SPAN = CORES * TILE
PAIR = 2
PAIRS = Z // PAIR
PLANE = Z * SPAN
STRIDE = PAIR * SPAN
HALF = GROUP * BLOCK
ROWS = PAIR * HALF
KEYS = PAIR * TILE
WIDE = 2 * HEAD_SIZE
HEAD_COLS = GROUP * HEAD_SIZE
BASE = (3, 1, 0, 2)
BLOCKS = X * PAIRS
NEVER = 1 << 20

EXP2_SCALE = math.log2(math.e) / math.sqrt(HEAD_SIZE)
START_MAX = -1e30
HIDDEN = -3e38
LARGEST_SUM = 2.0 ** 60


def square_groups():
    groups = []
    for k in range(X):
        for core in range(CORES):
            for y in range(Y):
                groups.append([(((BASE[z // PAIR] ^ k) * Z + z) * CORES + core) * Y + y for z in range(Z)])
    return groups


def base_of(pair):
    base = jnp.int32(BASE[-1])
    for p in range(PAIRS - 1):
        base = jnp.where(pair == p, BASE[p], base)
    return base


def line_groups(first):
    index = lambda x, z, core, y: ((x * Z + z) * CORES + core) * Y + y
    groups = []
    for z in range(Z):
        for core in range(CORES):
            if (core == 1) == first:
                groups += [[index(x, z, core, y) for x in range(X)] for y in range(Y)]
            else:
                groups += [[index(x, z, core, y) for y in range(Y)] for x in range(X)]
    return groups


def doc_start(bounds, position):
    start = jnp.zeros_like(position)
    for d in range(1, DOCS):
        start = jnp.where(bounds[d] <= position, bounds[d], start)
    return start


def mix(values, weights):
    return jnp.dot(values, weights.astype(jnp.bfloat16), preferred_element_type=jnp.float32)


def start_kernel(bounds, q_ref, rows_ref, top_ref, acc_ref):
    x, z, core, y = (lax.axis_index(a) for a in AXES)
    group = x ^ base_of(lax.div(z, PAIR))
    column = lax.broadcasted_iota(jnp.int32, (1, WIDE), 1)
    key_lanes = (column < HEAD_SIZE).astype(jnp.bfloat16)
    value_lanes = (column >= HEAD_SIZE).astype(jnp.bfloat16)
    row = lax.broadcasted_iota(jnp.int32, (1, ROWS), 1)
    row_offset = lax.div(row, HALF) * SPAN + lax.rem(row, BLOCK)

    def one_pair(p, _):
        first = (base_of(p) ^ group) * PLANE + p * STRIDE + core * TILE + y * BLOCK
        line = lax.broadcasted_iota(jnp.int32, (HEAD_SIZE, ROWS), 0)
        half = lax.broadcasted_iota(jnp.int32, (HEAD_SIZE, ROWS), 1) // HALF
        filler = ((line == 0) | (line == half + 1)).astype(jnp.bfloat16)
        own = [q_ref[PAIR * p + b] for b in range(PAIR)]
        pieces = []
        for block in own:
            turned = block[:, WIDE:].T
            pieces += [turned[j * HEAD_SIZE:(j + 1) * HEAD_SIZE] for j in range(GROUP)]
        rows = jnp.concatenate([jnp.concatenate(pieces, axis=1), filler], axis=0)
        rows_ref[p] = rows
        kv = jnp.concatenate([block[:, :WIDE] for block in own], axis=0)
        k = lax.broadcasted_iota(jnp.int32, (PAIR * BLOCK, 1), 0)
        k_offset = lax.div(k, BLOCK) * SPAN + lax.rem(k, BLOCK)
        scores = jnp.dot(kv * key_lanes, rows, preferred_element_type=jnp.float32)
        lo = doc_start(bounds, first + row_offset) - first
        scores = jnp.where((k_offset >= lo) & (k_offset <= row_offset), scores, HIDDEN)
        top = jnp.max(scores, axis=0, keepdims=True)
        top_ref[p] = top
        acc_ref[p] = mix((kv * value_lanes + key_lanes).T, jnp.exp2(scores * EXP2_SCALE - top * EXP2_SCALE))
        return 0

    lax.fori_loop(0, PAIRS, one_pair, 0)


def attention_kernel(stage, bounds, *refs):
    if stage == 0:
        rows_ref, top_ref, acc_in, own_ref, acc_out = refs
    else:
        rows_ref, top_ref, acc_in, own_ref, other_ref, out_ref, acc_ref, run_ref = refs
    x, z, core, y = (lax.axis_index(a) for a in AXES)
    mine = base_of(lax.div(z, PAIR))
    group = x ^ mine
    column = lax.broadcasted_iota(jnp.int32, (1, WIDE), 1)
    key_lanes = (column < HEAD_SIZE).astype(jnp.bfloat16)
    value_lanes = (column >= HEAD_SIZE).astype(jnp.bfloat16)
    row = lax.broadcasted_iota(jnp.int32, (1, ROWS), 1)
    row_offset = lax.div(row, HALF) * SPAN + lax.rem(row, BLOCK)
    key = lax.broadcasted_iota(jnp.int32, (KEYS, WIDE), 0)
    key_offset = lax.div(key, TILE) * SPAN + lax.rem(key, TILE)
    kv_ref, offset = (own_ref, core) if stage == 0 else (other_ref, 1 - core)

    def one_pair(p, _):
        plane = base_of(p) ^ group
        home = plane * PAIRS + p
        first = home * STRIDE + core * TILE + y * BLOCK
        start = doc_start(bounds, first)
        begin = lax.div(start, STRIDE)
        one_document = start == doc_start(bounds, first + SPAN + BLOCK - 1)

        after = jnp.where(column == HEAD_SIZE + 1, first, jnp.where(column == HEAD_SIZE + 2, first + SPAN, NEVER))
        held = jnp.where(column == HEAD_SIZE, first, NEVER)

        def load(kv_ref, offset, blocks, limits=None):
            parts, masks, origins = [], [], []
            for n, block in enumerate(blocks):
                near = jnp.minimum(block, BLOCKS - 1)
                q = lax.rem(near, PAIRS)
                source = lax.div(near, PAIRS) ^ base_of(q) ^ mine
                for g in range(PAIR):
                    for i in range(Y):
                        at = jnp.where(offset == 1, i * X + source, source * Y + i)
                        parts.append(kv_ref[at, q * PAIR + g])
                origin = block * STRIDE + offset * TILE
                origins.append(origin)
                if limits is not None:
                    before = jnp.where(column == HEAD_SIZE, limits[n] - origin, -NEVER)
                    unseen = (key_offset < before) | (key_offset >= after - origin)
                    if stage == 0:
                        unseen = unseen | ((key_offset >= held - origin) & (key_offset < held + BLOCK - origin))
                    masks.append(jnp.where(unseen, START_MAX, 0.0))
            kv = jnp.concatenate(parts, axis=0)
            keys = kv * key_lanes
            if limits is not None:
                keys = keys + jnp.concatenate(masks, axis=0).astype(jnp.bfloat16)
            return keys, (kv * value_lanes + key_lanes).T, origins

        def across(origins, low, high=None):
            offsets = jnp.concatenate([key_offset] * (ROWS // WIDE), axis=1)
            seen = []
            for origin in origins:
                inside = offsets >= low - origin
                seen.append(inside if high is None else inside & (offsets <= high - origin))
            return seen

        def hide(scores, seen):
            parts = [jnp.where(m, scores[n * KEYS:(n + 1) * KEYS], HIDDEN) for n, m in enumerate(seen)]
            return jnp.concatenate(parts, axis=0)

        if stage == 0:
            acc = acc_out.at[p]
        else:
            acc = acc_ref
        acc[...] = acc_in[p]

        def add(blocks, limits=None, lo=None):
            keys, values, origins = load(kv_ref, offset, blocks, limits)
            scores = jnp.dot(keys, rows_ref[p], preferred_element_type=jnp.float32)
            if lo is not None:
                scores = hide(scores, across(origins, lo))
            weights = jnp.exp2(scores * EXP2_SCALE - top_ref[p] * EXP2_SCALE)
            acc[...] += mix(values, weights)

        @pl.when(one_document)
        def _():
            inside = home - begin - 1
            many = inside >= 2

            @pl.when(many)
            def _():
                add([home, begin, begin + 1, begin + 2], [start] * 4)

            @pl.when(jnp.logical_not(many))
            def _():
                add([home, begin], [start, jnp.where(begin == home, NEVER, start)])

            taken = jnp.where(many, 2, 0)
            left = inside - taken
            base = begin + 1 + taken

            def step(s, _):
                add([base + 4 * s + n for n in range(4)])
                return 0

            lax.fori_loop(0, lax.div(left, 4), step, 0)

            @pl.when((left > 0) & (lax.rem(left, 4) >= 2))
            def _():
                at = base + left - lax.rem(left, 4)
                add([at, at + 1])

            @pl.when((left > 0) & (lax.rem(left, 2) == 1))
            def _():
                add([home - 1])

        @pl.when(jnp.logical_not(one_document))
        def _():
            lo = doc_start(bounds, first + row_offset)

            count = home - begin + 1

            def step(s, _):
                add([begin + 2 * s, begin + 2 * s + 1], [start, start], lo)
                return 0

            lax.fori_loop(0, lax.div(count, 2), step, 0)

            @pl.when(lax.rem(count, 2) == 1)
            def _():
                add([home], [start], lo)

        if stage == 0:
            return 0

        within = jnp.min((acc[0:1, :] <= LARGEST_SUM).astype(jnp.float32))

        @pl.when(within < 0.5)
        def _():
            hi = first + row_offset
            lo = doc_start(bounds, hi)
            acc[...] = jnp.zeros_like(acc)
            run_ref[...] = jnp.full(run_ref.shape, START_MAX, jnp.float32)
            for again_ref, again_offset in ((own_ref, core), (other_ref, 1 - core)):
                def step(block, _):
                    keys, values, origins = load(again_ref, again_offset, [block])
                    scores = jnp.dot(keys, rows_ref[p], preferred_element_type=jnp.float32)
                    scores = hide(scores, across(origins, lo, hi))
                    top = run_ref[...]
                    new_top = jnp.maximum(top, jnp.max(scores, axis=0, keepdims=True))
                    shrink = jnp.exp2((top - new_top) * EXP2_SCALE)
                    acc[...] = acc[...] * shrink + mix(values, jnp.exp2((scores - new_top) * EXP2_SCALE))
                    run_ref[...] = new_top
                    return 0

                lax.fori_loop(begin, home + 1, step, 0)

        result = (acc[HEAD_SIZE:, :] / acc[0:1, :]).T
        for b in range(PAIR):
            heads = [result[(b * GROUP + j) * BLOCK:(b * GROUP + j + 1) * BLOCK] for j in range(GROUP)]
            out_ref[PAIR * p + b] = jnp.concatenate(heads, axis=1).astype(jnp.bfloat16)
        return 0

    lax.fori_loop(0, PAIRS, one_pair, 0)


def pack_kernel(q_ref, k_ref, v_ref, out_ref):
    for h in range(KEY_VALUE_HEADS):
        cols = slice(h * HEAD_SIZE, (h + 1) * HEAD_SIZE)
        out_ref[h, :, :WIDE] = jnp.concatenate([k_ref[:, cols], v_ref[:, cols]], axis=1)
        out_ref[h, :, WIDE:] = q_ref[:, h * HEAD_COLS:(h + 1) * HEAD_COLS]


def on_device(queries, keys, values, doc_bounds):
    smem = pl.BlockSpec(memory_space=pltpu.SMEM)
    vmem = pl.BlockSpec(memory_space=pltpu.VMEM)
    groups = square_groups()
    packed = pl.pallas_call(
        pack_kernel,
        out_shape=pltpu.VMEM((Z, BLOCK, WIDE + HEAD_COLS), jnp.bfloat16),
        in_specs=[vmem] * 3,
        out_specs=vmem,
        name="pack",
    )(queries, keys, values)
    packed = lax.all_to_all(packed, AXES, 0, 0, axis_index_groups=groups, tiled=True)
    gathered = packed[:, :, :WIDE]
    for first in (True, False):
        copies = jnp.broadcast_to(gathered[None], (X,) + gathered.shape)
        gathered = lax.all_to_all(copies, AXES, 0, 0, axis_index_groups=line_groups(first), tiled=True)
    own = gathered.reshape(X * Y, Z, BLOCK, WIDE)
    other = lax.ppermute(own, "core", [(0, 1), (1, 0)])

    acc_shape = jax.ShapeDtypeStruct((PAIRS, WIDE, ROWS), jnp.float32)
    top_shape = jax.ShapeDtypeStruct((PAIRS, 1, ROWS), jnp.float32)
    rows_shape = jax.ShapeDtypeStruct((PAIRS, WIDE, ROWS), jnp.bfloat16)
    params = pltpu.CompilerParams(vmem_limit_bytes=40 * 1024 * 1024)
    rows, top, acc = pl.pallas_call(
        start_kernel,
        out_shape=tuple(pltpu.VMEM(a.shape, a.dtype) for a in (rows_shape, top_shape, acc_shape)),
        in_specs=[smem, vmem],
        out_specs=(vmem,) * 3,
        name="attention_start",
    )(doc_bounds, packed)
    acc = pl.pallas_call(
        functools.partial(attention_kernel, 0),
        out_shape=acc_shape,
        in_specs=[smem] + [vmem] * 4,
        out_specs=vmem,
        compiler_params=params,
        name="attention_own",
    )(doc_bounds, rows, top, acc, own)
    attended = pl.pallas_call(
        functools.partial(attention_kernel, 1),
        out_shape=jax.ShapeDtypeStruct((Z, BLOCK, HEAD_COLS), jnp.bfloat16),
        in_specs=[smem] + [vmem] * 5,
        out_specs=vmem,
        scratch_shapes=[pltpu.VMEM((WIDE, ROWS), jnp.float32), pltpu.VMEM((1, ROWS), jnp.float32)],
        compiler_params=params,
        name="attention_other",
    )(doc_bounds, rows, top, acc, own, other)
    attended = lax.all_to_all(attended, AXES, 0, 0, axis_index_groups=groups, tiled=True)
    return attended.transpose(1, 0, 2).reshape(BLOCK, QUERY_HEADS * HEAD_SIZE)


def solution(mesh):
    split = Mesh(mesh.devices.reshape(X, Z, CORES, Y), AXES)
    rows = P(AXES, None)
    return jax.shard_map(
        on_device,
        mesh=split,
        in_specs=(rows, rows, rows, P()),
        out_specs=rows,
        check_vma=False,
    )
```

```python
import functools
import math

import jax
import jax.numpy as jnp
from jax import lax
from jax.experimental import pallas as pl
from jax.experimental.pallas import tpu as pltpu
from jax.sharding import Mesh, PartitionSpec as P


QUERY_HEADS = 32
KEY_VALUE_HEADS = 8
HEAD_SIZE = 64
DOCS = 16
GROUP = QUERY_HEADS // KEY_VALUE_HEADS

X, Z, CORES, Y = 4, 8, 2, 4
AXES = ("x", "z", "core", "y")
BLOCK = 64
TILE = Y * BLOCK
SPAN = CORES * TILE
PAIR = 2
PAIRS = Z // PAIR
PLANE = Z * SPAN
STRIDE = PAIR * SPAN
HALF = GROUP * BLOCK
ROWS = PAIR * HALF
KEYS = PAIR * TILE
WIDE = 2 * HEAD_SIZE
SUMS = 16
MIXED = SUMS + HEAD_SIZE
HEAD_COLS = GROUP * HEAD_SIZE
BASE = (3, 1, 0, 2)
BLOCKS = X * PAIRS
NEVER = 1 << 20

EXP2_SCALE = math.log2(math.e) / math.sqrt(HEAD_SIZE)
START_MAX = -1e30
HIDDEN = -3e38
LARGEST_SUM = 2.0 ** 60


def square_groups():
    groups = []
    for k in range(X):
        for core in range(CORES):
            for y in range(Y):
                groups.append([(((BASE[z // PAIR] ^ k) * Z + z) * CORES + core) * Y + y for z in range(Z)])
    return groups


def base_of(pair):
    base = jnp.int32(BASE[-1])
    for p in range(PAIRS - 1):
        base = jnp.where(pair == p, BASE[p], base)
    return base


def line_groups(first):
    index = lambda x, z, core, y: ((x * Z + z) * CORES + core) * Y + y
    groups = []
    for z in range(Z):
        for core in range(CORES):
            if (core == 1) == first:
                groups += [[index(x, z, core, y) for x in range(X)] for y in range(Y)]
            else:
                groups += [[index(x, z, core, y) for y in range(Y)] for x in range(X)]
    return groups


def doc_start(bounds, position):
    start = jnp.zeros_like(position)
    for d in range(1, DOCS):
        start = jnp.where(bounds[d] <= position, bounds[d], start)
    return start


def mix(values, weights):
    return jnp.dot(values, weights.astype(jnp.bfloat16), preferred_element_type=jnp.float32)


def start_kernel(bounds, q_ref, rows_ref, top_ref, acc_ref):
    x, z, core, y = (lax.axis_index(a) for a in AXES)
    group = x ^ base_of(lax.div(z, PAIR))
    column = lax.broadcasted_iota(jnp.int32, (1, WIDE), 1)
    key_lanes = (column < HEAD_SIZE).astype(jnp.bfloat16)
    value_lanes = (column >= HEAD_SIZE).astype(jnp.bfloat16)
    row = lax.broadcasted_iota(jnp.int32, (1, ROWS), 1)
    row_offset = lax.div(row, HALF) * SPAN + lax.rem(row, BLOCK)

    def one_pair(p, _):
        first = (base_of(p) ^ group) * PLANE + p * STRIDE + core * TILE + y * BLOCK
        line = lax.broadcasted_iota(jnp.int32, (HEAD_SIZE, ROWS), 0)
        half = lax.broadcasted_iota(jnp.int32, (HEAD_SIZE, ROWS), 1) // HALF
        filler = ((line == 0) | (line == half + 1)).astype(jnp.bfloat16)
        own = [q_ref[PAIR * p + b] for b in range(PAIR)]
        pieces = []
        for block in own:
            turned = block[:, WIDE:].T
            pieces += [turned[j * HEAD_SIZE:(j + 1) * HEAD_SIZE] for j in range(GROUP)]
        rows = jnp.concatenate([jnp.concatenate(pieces, axis=1), filler], axis=0)
        rows_ref[p] = rows
        kv = jnp.concatenate([block[:, :WIDE] for block in own], axis=0)
        k = lax.broadcasted_iota(jnp.int32, (PAIR * BLOCK, 1), 0)
        k_offset = lax.div(k, BLOCK) * SPAN + lax.rem(k, BLOCK)
        scores = jnp.dot(kv * key_lanes, rows, preferred_element_type=jnp.float32)
        lo = doc_start(bounds, first + row_offset) - first
        scores = jnp.where((k_offset >= lo) & (k_offset <= row_offset), scores, HIDDEN)
        top = jnp.max(scores, axis=0, keepdims=True)
        top_ref[p] = top
        acc_ref[p] = mix((kv * value_lanes + key_lanes).T[WIDE - MIXED:], jnp.exp2(scores * EXP2_SCALE - top * EXP2_SCALE))
        return 0

    lax.fori_loop(0, PAIRS, one_pair, 0)


def attention_kernel(stage, bounds, *refs):
    if stage == 0:
        rows_ref, top_ref, acc_in, own_ref, acc_out = refs
    else:
        rows_ref, top_ref, acc_in, own_ref, other_ref, out_ref, acc_ref, run_ref = refs
    x, z, core, y = (lax.axis_index(a) for a in AXES)
    mine = base_of(lax.div(z, PAIR))
    group = x ^ mine
    column = lax.broadcasted_iota(jnp.int32, (1, WIDE), 1)
    key_lanes = (column < HEAD_SIZE).astype(jnp.bfloat16)
    value_lanes = (column >= HEAD_SIZE).astype(jnp.bfloat16)
    row = lax.broadcasted_iota(jnp.int32, (1, ROWS), 1)
    row_offset = lax.div(row, HALF) * SPAN + lax.rem(row, BLOCK)
    key = lax.broadcasted_iota(jnp.int32, (KEYS, WIDE), 0)
    key_offset = lax.div(key, TILE) * SPAN + lax.rem(key, TILE)
    kv_ref, offset = (own_ref, core) if stage == 0 else (other_ref, 1 - core)

    def one_pair(p, _):
        plane = base_of(p) ^ group
        home = plane * PAIRS + p
        first = home * STRIDE + core * TILE + y * BLOCK
        start = doc_start(bounds, first)
        begin = lax.div(start, STRIDE)
        one_document = start == doc_start(bounds, first + SPAN + BLOCK - 1)

        after = jnp.where(column == HEAD_SIZE + 1, first, jnp.where(column == HEAD_SIZE + 2, first + SPAN, NEVER))
        held = jnp.where(column == HEAD_SIZE, first, NEVER)

        def load(kv_ref, offset, blocks, limits=None):
            parts, masks, origins = [], [], []
            for n, block in enumerate(blocks):
                near = jnp.minimum(block, BLOCKS - 1)
                q = lax.rem(near, PAIRS)
                source = lax.div(near, PAIRS) ^ base_of(q) ^ mine
                for g in range(PAIR):
                    for i in range(Y):
                        at = jnp.where(offset == 1, i * X + source, source * Y + i)
                        parts.append(kv_ref[at, q * PAIR + g])
                origin = block * STRIDE + offset * TILE
                origins.append(origin)
                if limits is not None:
                    before = jnp.where(column == HEAD_SIZE, limits[n] - origin, -NEVER)
                    unseen = (key_offset < before) | (key_offset >= after - origin)
                    if stage == 0:
                        unseen = unseen | ((key_offset >= held - origin) & (key_offset < held + BLOCK - origin))
                    masks.append(jnp.where(unseen, START_MAX, 0.0))
            kv = jnp.concatenate(parts, axis=0)
            keys = kv * key_lanes
            if limits is not None:
                keys = keys + jnp.concatenate(masks, axis=0).astype(jnp.bfloat16)
            return keys, (kv * value_lanes + key_lanes).T[WIDE - MIXED:], origins

        def across(origins, low, high=None):
            offsets = jnp.concatenate([key_offset] * (ROWS // WIDE), axis=1)
            seen = []
            for origin in origins:
                inside = offsets >= low - origin
                seen.append(inside if high is None else inside & (offsets <= high - origin))
            return seen

        def hide(scores, seen):
            parts = [jnp.where(m, scores[n * KEYS:(n + 1) * KEYS], HIDDEN) for n, m in enumerate(seen)]
            return jnp.concatenate(parts, axis=0)

        if stage == 0:
            acc = acc_out.at[p]
        else:
            acc = acc_ref
        acc[...] = acc_in[p]

        def add(blocks, limits=None, lo=None):
            keys, values, origins = load(kv_ref, offset, blocks, limits)
            scores = jnp.dot(keys, rows_ref[p], preferred_element_type=jnp.float32)
            if lo is not None:
                scores = hide(scores, across(origins, lo))
            weights = jnp.exp2(scores * EXP2_SCALE - top_ref[p] * EXP2_SCALE)
            acc[...] += mix(values, weights)

        @pl.when(one_document)
        def _():
            inside = home - begin - 1
            many = inside >= 2

            @pl.when(many)
            def _():
                add([home, begin, begin + 1, begin + 2], [start] * 4)

            @pl.when(jnp.logical_not(many))
            def _():
                add([home, begin], [start, jnp.where(begin == home, NEVER, start)])

            taken = jnp.where(many, 2, 0)
            left = inside - taken
            base = begin + 1 + taken

            def step(s, _):
                add([base + 4 * s + n for n in range(4)])
                return 0

            lax.fori_loop(0, lax.div(left, 4), step, 0)

            @pl.when((left > 0) & (lax.rem(left, 4) >= 2))
            def _():
                at = base + left - lax.rem(left, 4)
                add([at, at + 1])

            @pl.when((left > 0) & (lax.rem(left, 2) == 1))
            def _():
                add([home - 1])

        @pl.when(jnp.logical_not(one_document))
        def _():
            lo = doc_start(bounds, first + row_offset)

            count = home - begin + 1

            def step(s, _):
                add([begin + 2 * s, begin + 2 * s + 1], [start, start], lo)
                return 0

            lax.fori_loop(0, lax.div(count, 2), step, 0)

            @pl.when(lax.rem(count, 2) == 1)
            def _():
                add([home], [start], lo)

        if stage == 0:
            return 0

        within = jnp.min((acc[0:1, :] <= LARGEST_SUM).astype(jnp.float32))

        @pl.when(within < 0.5)
        def _():
            hi = first + row_offset
            lo = doc_start(bounds, hi)
            acc[...] = jnp.zeros_like(acc)
            run_ref[...] = jnp.full(run_ref.shape, START_MAX, jnp.float32)
            for again_ref, again_offset in ((own_ref, core), (other_ref, 1 - core)):
                def step(block, _):
                    keys, values, origins = load(again_ref, again_offset, [block])
                    scores = jnp.dot(keys, rows_ref[p], preferred_element_type=jnp.float32)
                    scores = hide(scores, across(origins, lo, hi))
                    top = run_ref[...]
                    new_top = jnp.maximum(top, jnp.max(scores, axis=0, keepdims=True))
                    shrink = jnp.exp2((top - new_top) * EXP2_SCALE)
                    acc[...] = acc[...] * shrink + mix(values, jnp.exp2((scores - new_top) * EXP2_SCALE))
                    run_ref[...] = new_top
                    return 0

                lax.fori_loop(begin, home + 1, step, 0)

        result = (acc[SUMS:, :] / acc[0:1, :]).T
        for b in range(PAIR):
            heads = [result[(b * GROUP + j) * BLOCK:(b * GROUP + j + 1) * BLOCK] for j in range(GROUP)]
            out_ref[PAIR * p + b] = jnp.concatenate(heads, axis=1).astype(jnp.bfloat16)
        return 0

    lax.fori_loop(0, PAIRS, one_pair, 0)


def pack_kernel(q_ref, k_ref, v_ref, out_ref):
    for h in range(KEY_VALUE_HEADS):
        cols = slice(h * HEAD_SIZE, (h + 1) * HEAD_SIZE)
        out_ref[h, :, :WIDE] = jnp.concatenate([k_ref[:, cols], v_ref[:, cols]], axis=1)
        out_ref[h, :, WIDE:] = q_ref[:, h * HEAD_COLS:(h + 1) * HEAD_COLS]


def on_device(queries, keys, values, doc_bounds):
    smem = pl.BlockSpec(memory_space=pltpu.SMEM)
    vmem = pl.BlockSpec(memory_space=pltpu.VMEM)
    groups = square_groups()
    packed = pl.pallas_call(
        pack_kernel,
        out_shape=pltpu.VMEM((Z, BLOCK, WIDE + HEAD_COLS), jnp.bfloat16),
        in_specs=[vmem] * 3,
        out_specs=vmem,
        name="pack",
    )(queries, keys, values)
    packed = lax.all_to_all(packed, AXES, 0, 0, axis_index_groups=groups, tiled=True)
    gathered = packed[:, :, :WIDE]
    for first in (True, False):
        copies = jnp.broadcast_to(gathered[None], (X,) + gathered.shape)
        gathered = lax.all_to_all(copies, AXES, 0, 0, axis_index_groups=line_groups(first), tiled=True)
    own = gathered.reshape(X * Y, Z, BLOCK, WIDE)
    other = lax.ppermute(own, "core", [(0, 1), (1, 0)])

    acc_shape = jax.ShapeDtypeStruct((PAIRS, MIXED, ROWS), jnp.float32)
    top_shape = jax.ShapeDtypeStruct((PAIRS, 1, ROWS), jnp.float32)
    rows_shape = jax.ShapeDtypeStruct((PAIRS, WIDE, ROWS), jnp.bfloat16)
    params = pltpu.CompilerParams(vmem_limit_bytes=40 * 1024 * 1024)
    rows, top, acc = pl.pallas_call(
        start_kernel,
        out_shape=tuple(pltpu.VMEM(a.shape, a.dtype) for a in (rows_shape, top_shape, acc_shape)),
        in_specs=[smem, vmem],
        out_specs=(vmem,) * 3,
        name="attention_start",
    )(doc_bounds, packed)
    acc = pl.pallas_call(
        functools.partial(attention_kernel, 0),
        out_shape=acc_shape,
        in_specs=[smem] + [vmem] * 4,
        out_specs=vmem,
        compiler_params=params,
        name="attention_own",
    )(doc_bounds, rows, top, acc, own)
    attended = pl.pallas_call(
        functools.partial(attention_kernel, 1),
        out_shape=jax.ShapeDtypeStruct((Z, BLOCK, HEAD_COLS), jnp.bfloat16),
        in_specs=[smem] + [vmem] * 5,
        out_specs=vmem,
        scratch_shapes=[pltpu.VMEM((MIXED, ROWS), jnp.float32), pltpu.VMEM((1, ROWS), jnp.float32)],
        compiler_params=params,
        name="attention_other",
    )(doc_bounds, rows, top, acc, own, other)
    attended = lax.all_to_all(attended, AXES, 0, 0, axis_index_groups=groups, tiled=True)
    return attended.transpose(1, 0, 2).reshape(BLOCK, QUERY_HEADS * HEAD_SIZE)


def solution(mesh):
    split = Mesh(mesh.devices.reshape(X, Z, CORES, Y), AXES)
    rows = P(AXES, None)
    return jax.shard_map(
        on_device,
        mesh=split,
        in_specs=(rows, rows, rows, P()),
        out_specs=rows,
        check_vma=False,
    )
```
